128 devices in a mesh: dp: 16 (over y, z_lo, core), tp: 8 (over x, z_hi).
Axes of the slice: x: 4, y: 4, z: 4 (z_hi: 2, z_lo: 2; z = z_hi * 2 + z_lo), core: 2. Of those that a mesh axis runs over, the one named last changes fastest.
Arguments:
- x_tokens: bfloat16 [16384, 8192], P(('dp', 'tp')), may hold values from -24 to 24
- segment_ids: int32 [16, 1024], P('dp'), may hold values from 0 to 3, never falling along the last dimension, each value on 1 to 512 neighbouring positions
- attended_grad: bfloat16 [16384, 4096], P('dp', 'tp'), may hold values from -6 to 6
- norm_gain: float32 [8192], replicated, may hold values from 0.1 to 1.9
- w_query: bfloat16 [8192, 4096], P(None, 'tp'), may hold values from -1 to 1
- w_key: bfloat16 [8192, 1024], P(None, 'tp'), may hold values from -4 to 4
- w_value: bfloat16 [8192, 1024], P(None, 'tp'), may hold values from -0.0625 to 0.0625
Outputs:
- attended: bfloat16 [16384, 4096], P('dp', 'tp')
- input_grad: bfloat16 [16384, 8192], P(('dp', 'tp'))
- gain_grad: float32 [8192], replicated
- grad_query: float32 [8192, 4096], P('dp', 'tp')
- grad_key: float32 [8192, 1024], P('dp', 'tp')
- grad_value: float32 [8192, 1024], P('dp', 'tp')
The draws below stay inside these ranges and needn't reach their ends.
Inputs may be any that keep to these rules, and one draw needn't show every extreme that they name: `segment_ids`: along each replica's row the numbers never fall; every number 0 to 3 covers one run of 1 to 512 positions.
All inputs are finite; a program needn't handle non-finite values.
Results may differ from the reference program's by a relative error of at most 0.028.
The reference program's roundings to bfloat16 on the way count: a program that leaves them out, or rounds other values in their place, can miss the bound.
Values may be sent and summed in bfloat16 or wider, within the bound.
A program may use at most 256 MiB of HBM per device.

```python
import math
import jax
import jax.numpy as jnp
import numpy as np
from jax import lax

D = 8192
QH = 32
KVH = 8
HD = 128
SEQ = 1024
TOKENS = 16384
N_DP = 16
N_TP = 8


def query_matrix(key):
    raw = jax.random.normal(jax.random.fold_in(key, 11), (D, QH * HD), jnp.float32) / math.sqrt(D)
    return jnp.clip(raw, -1.0, 1.0)


def draw_w_query(key, part):
    return query_matrix(key).astype(jnp.bfloat16)


def draw_w_key(key, part):
    noise = jax.random.normal(jax.random.fold_in(key, 12), (D, KVH * HD), jnp.float32) / math.sqrt(D)
    return jnp.clip(noise, -4.0, 4.0).astype(jnp.bfloat16)


def spiked(result, key, source, target, shards_of, factor):
    owner, partner = [(jnp.arange(result.shape[dim]) // (result.shape[dim] // shards_of)).reshape([-1 if axis == dim else 1 for axis in range(result.ndim)]) for dim in (source, target)]
    chosen = jax.random.permutation(key, shards_of)[partner]
    strong = (owner == chosen) | (owner == (partner + shards_of // 2) % shards_of)
    return jnp.where(strong, factor * result, result)


def block_scale(stream_key, extent, pieces, smallest, top_value):
    gain, own = 1.0, jax.random.fold_in(stream_key, 6)
    for axis_at, blocks in pieces:
        heights = jnp.exp(jax.random.uniform(jax.random.fold_in(own, axis_at), (blocks,), jnp.float32, smallest / len(pieces), top_value / len(pieces)))
        gain = gain * jnp.repeat(heights, extent[axis_at] // blocks).reshape([-1 if axis == axis_at else 1 for axis in range(len(extent))])
    return gain


def profile(count, total, bound, skew):
    portions = [(1 << 20) // math.isqrt(grade ** skew) + 1 for grade in range(2, count + 1)]
    rest, counts = total - bound - (count - 1), [1] * (count - 1)
    while rest > 0:
        movable = [i for i in range(count - 1) if counts[i] < bound]
        whole, remaining = sum([portions[i] for i in movable]), rest
        for i in movable:
            addition = min(bound - counts[i], max(1, remaining * portions[i] // whole), rest)
            counts[i] = counts[i] + addition
            rest = rest - addition
    return np.array([bound] + counts)


def uneven_parts(stream_key, amount, total, limit, lean):
    if amount == 2:
        one = jax.random.randint(stream_key, (), max(1, total - limit), min(limit, total - 1) + 1)
        return jnp.stack([one, total - one])
    tallies = jnp.asarray(profile(amount, total, limit, lean), jnp.int32)
    pairs = (amount - 1) // 2
    source_of, receiver = tallies[1:1 + 2 * pairs:2], tallies[2:2 + 2 * pairs:2]
    room = jnp.minimum(source_of - 1, limit - receiver)
    moved = jax.random.randint(jax.random.fold_in(stream_key, 1), (pairs,), 0, 1 << 20) % (room + 1)
    tallies = tallies.at[1:1 + 2 * pairs:2].set(source_of - moved).at[2:2 + 2 * pairs:2].set(receiver + moved)
    return tallies[jax.random.permutation(jax.random.fold_in(stream_key, 2), amount)]


def gaussian(stream_key, extent, width, limit, shards=(), kind=jnp.bfloat16):
    loudness = block_scale(stream_key, extent, shards, -0.22, 0.18) if shards else 1.0
    entries = jax.random.normal(stream_key, extent, jnp.float32) * width * loudness
    return jnp.minimum(jnp.maximum(entries, -limit), limit).astype(kind)


def heavy_noise(key, shape, deviation, bound, shards, heavy, kind=jnp.bfloat16):
    drawn = deviation * jax.random.normal(key, shape, jnp.float32)
    if shards:
        drawn = drawn * block_scale(key, shape, shards, -0.22, 0.18)
    return jnp.clip(spiked(drawn, jax.random.fold_in(key, 3), *heavy), -bound, bound).astype(kind)


def setup_inputs(seed: int = 0) -> dict:
    keys = jax.random.split(jax.random.key(seed), 8)
    return {
        "x_tokens": heavy_noise(keys[0], (TOKENS, D), 1.0, 24.0, ((0, 128),), (0, 1, 128, 5.5)),
        "segment_ids": jax.vmap(lambda own: jnp.searchsorted(jnp.cumsum(uneven_parts(own, 4, SEQ, SEQ // 2, 1)), jnp.arange(SEQ), side="right"))(jax.random.split(keys[1], N_DP)).reshape((N_DP, SEQ)).astype(jnp.int32),
        "attended_grad": gaussian(keys[2], (TOKENS, QH * HD), 1.0, 6.0, ((0, 16), (1, 8))),
        "norm_gain": jnp.clip(1.0 + 0.18 * jax.random.normal(keys[3], (D,), jnp.float32), 0.1, 1.9),
        "w_query": draw_w_query(jax.random.fold_in(keys[7], 71), 0),
        "w_key": draw_w_key(jax.random.fold_in(keys[7], 71), 0),
        "w_value": gaussian(keys[6], (D, KVH * HD), D ** -0.5, 0.0625, ((1, 8),)),
    }


epsilon = 1e-05
rope_base = 500000.0

def rope_tables(segment_row):
    length = segment_row.shape[0]
    earlier = (segment_row[None, :] < segment_row[:, None]).astype(jnp.int32)
    offset = jnp.arange(length, dtype=jnp.int32) - lax.optimization_barrier(jnp.sum(earlier, axis=1)).astype(jnp.int32)
    half_dim = HD // 2
    inverse_freq = rope_base ** (-(jnp.arange(half_dim, dtype=jnp.float32) * 2.0 / HD))
    angle = offset.astype(jnp.float32)[:, None] * inverse_freq[None, :]
    return (jnp.cos(angle)[:, None, :], jnp.sin(angle)[:, None, :])

def attend_mask(segment_row):
    length = segment_row.shape[0]
    position = jnp.arange(length, dtype=jnp.int32)
    return (position[None, :] <= position[:, None]) & (segment_row[None, :] == segment_row[:, None])

def apply_rope(head_rows, cosine_table, sine_table, direction):
    half_dim = head_rows.shape[-1] // 2
    first_half = head_rows[..., :half_dim]
    second_half = head_rows[..., half_dim:]
    return jnp.concatenate([first_half * cosine_table - direction * second_half * sine_table, second_half * cosine_table + direction * first_half * sine_table], axis=-1)

def group_sum(left_parts, right_parts):
    lefts = jnp.concatenate([part.reshape(SEQ, N_TP, -1) for part in left_parts], axis=2).astype(jnp.float32)
    rights = jnp.concatenate([part.reshape(N_TP, -1, D) for part in right_parts], axis=1).astype(jnp.float32)
    partial_sums = jnp.einsum('sgc,gcd->gsd', lefts, rights)
    rounded = lax.optimization_barrier(partial_sums.astype(jnp.bfloat16))
    return lax.optimization_barrier(jnp.sum(rounded.astype(jnp.float32), axis=0))

def replica(x_rows, segment_row, grad_rows, norm_gain, w_query, w_key, w_value):
    group = QH // KVH
    score_scale = float(HD) ** (-0.5)
    as_float = x_rows.astype(jnp.float32)
    inverse = lax.rsqrt(lax.optimization_barrier(jnp.mean(as_float * as_float, axis=1, keepdims=True)) + epsilon)
    x_hat = as_float * inverse
    normed = (x_hat * norm_gain).astype(jnp.bfloat16)
    cosine_table, sine_table = rope_tables(segment_row)
    allowed = attend_mask(segment_row)
    query_f = jnp.dot(normed, w_query, preferred_element_type=jnp.float32).reshape(SEQ, QH, HD)
    queries = apply_rope(query_f, cosine_table, sine_table, 1.0).astype(jnp.bfloat16)
    key_f = jnp.dot(normed, w_key, preferred_element_type=jnp.float32).reshape(SEQ, KVH, HD)
    key_rows = apply_rope(key_f, cosine_table, sine_table, 1.0).astype(jnp.bfloat16)
    values_in = jnp.dot(normed, w_value, preferred_element_type=jnp.float32).astype(jnp.bfloat16).reshape(SEQ, KVH, HD)
    grouped = queries.reshape(SEQ, KVH, group, HD).astype(jnp.float32)
    scores = jnp.einsum('skgd,tkd->kgst', grouped, key_rows.astype(jnp.float32)) * score_scale
    scores = jnp.where(allowed[None, None], scores, -1e+30)
    highest = lax.optimization_barrier(jnp.max(scores, axis=3, keepdims=True))
    exponent = jnp.exp(scores - highest)
    probability = exponent / lax.optimization_barrier(jnp.sum(exponent, axis=3, keepdims=True))
    weights_b = probability.astype(jnp.bfloat16)
    attended = jnp.einsum('kgst,tkd->skgd', weights_b.astype(jnp.float32), values_in.astype(jnp.float32)).astype(jnp.bfloat16)
    attended_flat = attended.reshape(SEQ, QH * HD)
    out_grouped = grad_rows.reshape(SEQ, KVH, group, HD).astype(jnp.float32)
    row_delta = lax.optimization_barrier(jnp.sum(out_grouped * attended.astype(jnp.float32), axis=3))
    value_d = jnp.einsum('kgst,skgd->tkd', weights_b.astype(jnp.float32), out_grouped).astype(jnp.bfloat16)
    prob_d = jnp.einsum('skgd,tkd->kgst', out_grouped, values_in.astype(jnp.float32))
    score_d = (probability * (prob_d - jnp.transpose(row_delta, (1, 2, 0))[..., None]) * score_scale).astype(jnp.bfloat16)
    query_rot = jnp.einsum('kgst,tkd->skgd', score_d.astype(jnp.float32), key_rows.astype(jnp.float32)).reshape(SEQ, QH, HD)
    key_rot = jnp.einsum('kgst,skgd->tkd', score_d.astype(jnp.float32), grouped)
    query_d = apply_rope(query_rot, cosine_table, sine_table, -1.0).astype(jnp.bfloat16).reshape(SEQ, QH * HD)
    key_d = apply_rope(key_rot, cosine_table, sine_table, -1.0).astype(jnp.bfloat16).reshape(SEQ, KVH * HD)
    value_flat = value_d.reshape(SEQ, KVH * HD)
    normed_d = group_sum([query_d, key_d, value_flat], [w_query.T, w_key.T, w_value.T])
    scaled_d = normed_d * norm_gain
    input_grad = (inverse * (scaled_d - x_hat * lax.optimization_barrier(jnp.mean(scaled_d * x_hat, axis=1, keepdims=True)))).astype(jnp.bfloat16)
    gain_term = lax.optimization_barrier(jnp.sum(normed_d * x_hat, axis=0))
    grads = (jnp.dot(normed.T, query_d, preferred_element_type=jnp.float32).astype(jnp.bfloat16), jnp.dot(normed.T, key_d, preferred_element_type=jnp.float32).astype(jnp.bfloat16), jnp.dot(normed.T, value_flat, preferred_element_type=jnp.float32).astype(jnp.bfloat16))
    return (attended_flat, input_grad, gain_term, grads)

def reference(x_tokens, segment_ids, attended_grad, norm_gain, w_query, w_key, w_value):
    x_blocks = x_tokens.reshape(N_DP, SEQ, D)
    grad_blocks = attended_grad.reshape(N_DP, SEQ, QH * HD)
    initial = (jnp.zeros((D, QH * HD), jnp.float32), jnp.zeros((D, KVH * HD), jnp.float32), jnp.zeros((D, KVH * HD), jnp.float32), jnp.zeros((D,), jnp.float32))

    def replica_step(running, inputs):
        x_rows, segment_row, grad_rows = inputs
        attended_flat, input_grad, gain_term, grads = replica(x_rows, segment_row, grad_rows, norm_gain, w_query, w_key, w_value)
        grads = lax.optimization_barrier(grads)
        summed = tuple((total + grad.astype(jnp.float32) for total, grad in zip(running[:3], grads)))
        return (summed + (running[3] + gain_term,), (attended_flat, input_grad))
    totals, (outputs, input_grads) = lax.scan(replica_step, initial, (x_blocks, segment_ids, grad_blocks))
    return (outputs.reshape(N_DP * SEQ, QH * HD), input_grads.reshape(N_DP * SEQ, D), totals[3], totals[0], totals[1], totals[2])
```

```python
import jax
import jax.numpy as jnp
from jax import lax
from jax.experimental import pallas as pl
from jax.experimental.pallas import tpu as pltpu
from jax.sharding import Mesh
from jax.sharding import PartitionSpec as P

HD = 128
SPLIT = 4608
MESH = pl.DeviceIdType.MESH
TP = ("x", "zh")
DP = ("y", "zl", "c")
DP_TP = ("y", "zl", "c", "x", "zh")
epsilon = 1e-05
rope_base = 500000.0
def gather_kernel(n_ref, wq_ref, wk_ref, wv_ref, qkv_ref, full_ref, a_s, w_s, send, recv, local):
    x=lax.axis_index("x"); z=lax.axis_index("zh")
    right=lax.rem(x+1,4); left=lax.rem(x+3,4); far=lax.rem(x+2,4)
    to_right={"x":right}; to_left={"x":left}; to_z={"zh":1-z}
    half=a_s.shape[2]; rows=2*half
    lo=pl.ds(0,SPLIT); hi=pl.ds(SPLIT,a_s.shape[3]-SPLIT); every=pl.ds(0,a_s.shape[3])
    own=pltpu.make_async_copy(n_ref,a_s.at[2*x+z],local.at[0]); own.start()
    bar=pltpu.get_barrier_semaphore()
    for dev in (to_right,to_left,to_z):
        pl.semaphore_signal(bar,inc=1,device_id=dev,device_id_type=MESH)
    own.wait()
    pl.semaphore_wait(bar,3)
    wide=wq_ref.shape[1]; narrow=wk_ref.shape[1]
    loads=[pltpu.make_async_copy(wq_ref,w_s.at[:,pl.ds(0,wide)],local.at[1]),
           pltpu.make_async_copy(wk_ref,w_s.at[:,pl.ds(wide,narrow)],local.at[2]),
           pltpu.make_async_copy(wv_ref,w_s.at[:,pl.ds(wide+narrow,narrow)],local.at[3])]
    sent=[]
    def copy(k,sx,sz,h,cols,dev):
        ref=a_s.at[2*sx+sz,h,:,cols]
        return pltpu.make_async_remote_copy(src_ref=ref,dst_ref=ref,send_sem=send.at[k],recv_sem=recv.at[k],device_id=dev,device_id_type=MESH)
    def go(k,sx,sz,h,cols,dev):
        c=copy(k,sx,sz,h,cols,dev); c.start(); sent.append(c)
    def got(k,sx,sz,h,cols):
        copy(k,sx,sz,h,cols,to_z).wait_recv()
    o=1-z
    go(0,x,z,0,every,to_right); go(1,x,z,1,every,to_left)
    go(6,x,z,0,lo,to_z); go(7,x,z,1,lo,to_z)
    go(2,x,z,1,every,to_right); go(3,x,z,0,every,to_left)
    go(8,x,z,0,hi,to_z); go(9,x,z,1,hi,to_z)
    for c in loads: c.start()
    outs=[]
    def done(i,sx,sz):
        c=pltpu.make_async_copy(a_s.at[2*sx+sz],full_ref.at[2*sx+sz],local.at[4+i]); c.start(); outs.append(c)
    def project(slots):
        def one(i,_):
            s=slots(i)
            r=pl.ds(pl.multiple_of(s*rows,rows),rows)
            def part(j,_):
                kk=pl.ds(pl.multiple_of(j*KC,KC),KC)
                p=lax.dot_general(a_s[s,:,:,kk].reshape(rows,KC),w_s[kk,:],(((1,),(0,)),((),())),preferred_element_type=jnp.float32)
                qkv_ref[r,:]=jnp.where(j==0,p,qkv_ref[r,:]+p)
                return 0
            lax.fori_loop(0,a_s.shape[3]//KC,part,0)
            return 0
        return one
    KC=2048
    def run(n,f): lax.fori_loop(0,n,project(f),0)
    done(0,x,z)
    for c in loads: c.wait()
    run(1,lambda i: 2*x+z)
    got(0,left,z,0,every); go(4,left,z,0,every,to_right); go(10,left,z,0,hi,to_z)
    got(1,right,z,1,every); go(5,right,z,1,every,to_left); go(11,right,z,1,hi,to_z)
    got(6,x,o,0,lo); go(12,x,o,0,lo,to_right); got(7,x,o,1,lo); go(13,x,o,1,lo,to_left)
    go(14,x,o,1,lo,to_right); go(15,x,o,0,lo,to_left)
    got(2,left,z,1,every); go(16,left,z,1,hi,to_z)
    got(3,right,z,0,every); go(17,right,z,0,hi,to_z)
    done(1,left,z); done(2,right,z)
    got(8,x,o,0,hi); got(9,x,o,1,hi); done(3,x,o)
    run(2,lambda i: 2*lax.rem(x+1+2*i,4)+z)
    got(4,far,z,0,every); go(18,far,z,0,hi,to_z)
    got(5,far,z,1,every); go(19,far,z,1,hi,to_z)
    done(4,far,z)
    run(1,lambda i: 2*x+o)
    got(12,left,o,0,lo); go(20,left,o,0,lo,to_right)
    got(13,right,o,1,lo); go(21,right,o,1,lo,to_left)
    run(1,lambda i: 2*far+z)
    got(10,left,o,0,hi); got(11,right,o,1,hi)
    got(14,left,o,1,lo); got(16,left,o,1,hi); done(5,left,o)
    got(15,right,o,0,lo); got(17,right,o,0,hi); done(6,right,o)
    run(2,lambda i: 2*lax.rem(x+1+2*i,4)+o)
    got(20,far,o,0,lo); got(21,far,o,1,lo); got(18,far,o,0,hi); got(19,far,o,1,hi); done(7,far,o)
    run(1,lambda i: 2*far+o)
    for c in sent: c.wait_send()
    for c in outs: c.wait()

def gather_project(normed,wq,wk,wv):
    rows,feat=normed.shape
    cols=wq.shape[1]+2*wk.shape[1]
    any_=pl.BlockSpec(memory_space=pl.ANY); vm=pl.BlockSpec(memory_space=pltpu.VMEM)
    qkv,full=pl.pallas_call(gather_kernel,
        out_shape=(jax.ShapeDtypeStruct((8*rows,cols),jnp.float32),jax.ShapeDtypeStruct((8,2,rows//2,feat),jnp.bfloat16)),
        in_specs=[any_]*4,out_specs=(vm,any_),
        scratch_shapes=[pltpu.VMEM((8,2,rows//2,feat),jnp.bfloat16),pltpu.VMEM((feat,cols),jnp.bfloat16),
            pltpu.SemaphoreType.DMA((22,)),pltpu.SemaphoreType.DMA((22,)),pltpu.SemaphoreType.DMA((12,))],
        compiler_params=pltpu.CompilerParams(collective_id=1,has_side_effects=True,vmem_limit_bytes=60*2**20),name="gather_project",
        cost_estimate=pl.CostEstimate(flops=2*8*rows*feat*cols,bytes_accessed=48*2**20,transcendentals=0),
    )(normed.reshape(2,rows//2,feat),wq,wk,wv)
    return qkv,full.reshape(8*rows,feat)
BQ=256
def _nt(a,b): return lax.dot_general(a,b,(((1,),(1,)),((),())),preferred_element_type=jnp.float32)
def _tn(a,b): return lax.dot_general(a,b,(((0,),(0,)),((),())),preferred_element_type=jnp.float32)
def _nn(a,b): return lax.dot_general(a,b,(((1,),(0,)),((),())),preferred_element_type=jnp.float32)

def attention_kernel(qkv_ref, go_ref, cos_ref, sin_ref, segr_ref, segc_ref, att_ref, d_ref, q_s, k_s, v_s, dk_s, dv_s):
    seq=qkv_ref.shape[0]; heads=go_ref.shape[1]//HD; width=heads*HD
    scale=float(HD)**-0.5
    def rope(u,c,s): return u*c+pltpu.roll(u,HD//2,1)*s
    nb=seq//BQ
    for b in range(nb):
        r=slice(b*BQ,(b+1)*BQ)
        c=cos_ref[r,:]; s=sin_ref[r,:]
        for h in range(heads):
            q_s[r,h*HD:(h+1)*HD]=rope(qkv_ref[r,h*HD:(h+1)*HD],c,s).astype(jnp.bfloat16)
        k_s[r,:]=rope(qkv_ref[r,width:width+HD],c,s).astype(jnp.bfloat16)
        v_s[r,:]=qkv_ref[r,width+HD:width+2*HD].astype(jnp.bfloat16)
    dk_s[...]=jnp.zeros_like(dk_s)
    dv_s[...]=jnp.zeros_like(dv_s)
    for b in range(nb):
        r=slice(b*BQ,(b+1)*BQ)
        lo=max(0,(b*BQ-511)//BQ*BQ); hi=(b+1)*BQ
        kr=slice(lo,hi)
        rows=lax.broadcasted_iota(jnp.int32,(BQ,hi-lo),0)+b*BQ
        cols=lax.broadcasted_iota(jnp.int32,(BQ,hi-lo),1)+lo
        mask=(cols<=rows)&(segr_ref[0:1,kr]==segc_ref[r,0:1])
        def head(h,_):
            hs=pl.ds(pl.multiple_of(h*HD,HD),HD)
            q=q_s[r,hs]; go=go_ref[r,hs]
            k=k_s[kr,:]; v=v_s[kr,:]
            sc=jnp.where(mask,_nt(q,k)*scale,-1e30)
            m=jnp.max(sc,axis=1,keepdims=True)
            e=jnp.exp(sc-m)
            p=e*(1.0/jnp.sum(e,axis=1,keepdims=True))
            w=p.astype(jnp.bfloat16)
            o=_nn(w,v).astype(jnp.bfloat16)
            att_ref[r,hs]=o
            delta=jnp.sum(go.astype(jnp.float32)*o.astype(jnp.float32),axis=1,keepdims=True)
            dv_s[kr,:]+=_tn(w,go)
            dp=_nt(go,v)
            ds=(p*(dp-delta)*scale).astype(jnp.bfloat16)
            dq=_nn(ds,k)
            d_ref[r,hs]=rope(dq,cos_ref[r,:],-sin_ref[r,:]).astype(jnp.bfloat16)
            dk_s[kr,:]+=_tn(ds,q)
            return 0
        lax.fori_loop(0,heads,head,0,unroll=True)
    d_ref[:,width:width+HD]=rope(dk_s[...],cos_ref[...],-sin_ref[...]).astype(jnp.bfloat16)
    d_ref[:,width+HD:width+2*HD]=dv_s[...].astype(jnp.bfloat16)

def attention(qkv,go,cos,sin,segs):
    seq=qkv.shape[0]
    vm=pl.BlockSpec(memory_space=pltpu.VMEM)
    return pl.pallas_call(attention_kernel,
        out_shape=(jax.ShapeDtypeStruct(go.shape,jnp.bfloat16),jax.ShapeDtypeStruct(qkv.shape,jnp.bfloat16)),
        in_specs=[vm]*6,out_specs=(vm,vm),
        scratch_shapes=[pltpu.VMEM(go.shape,jnp.bfloat16),pltpu.VMEM((seq,HD),jnp.bfloat16),pltpu.VMEM((seq,HD),jnp.bfloat16),pltpu.VMEM((seq,HD),jnp.float32),pltpu.VMEM((seq,HD),jnp.float32)],
        compiler_params=pltpu.CompilerParams(vmem_limit_bytes=60*2**20),name="attention",
        cost_estimate=pl.CostEstimate(flops=12*go.shape[1]*seq*seq//2,bytes_accessed=12*2**20,transcendentals=0),
    )(qkv,go,cos,sin,segs.reshape(1,seq),segs.reshape(seq,1))
CC=512
def scatter_kernel(d_ref, wq_ref, wk_ref, wv_ref, out_ref, w_s, po, pw, ro, rw, rq, rp, send, recv, local):
    x=lax.axis_index("x"); z=lax.axis_index("zh"); o=1-z
    right=lax.rem(x+1,4); left=lax.rem(x+3,4); far=lax.rem(x+2,4)
    to_right={"x":right}; to_left={"x":left}; to_z={"zh":o}
    feat=po.shape[3]; half=po.shape[2]; rows=2*half
    lo=pl.ds(0,SPLIT); hi=pl.ds(SPLIT,feat-SPLIT); every=pl.ds(0,feat)
    wide=wq_ref.shape[1]; narrow=wk_ref.shape[1]
    loads=[pltpu.make_async_copy(wq_ref,w_s.at[:,pl.ds(0,wide)],local.at[0]),
           pltpu.make_async_copy(wk_ref,w_s.at[:,pl.ds(wide,narrow)],local.at[1]),
           pltpu.make_async_copy(wv_ref,w_s.at[:,pl.ds(wide+narrow,narrow)],local.at[2])]
    for c in loads: c.start()
    bar=pltpu.get_barrier_semaphore()
    for dev in (to_right,to_left,to_z):
        pl.semaphore_signal(bar,inc=1,device_id=dev,device_id_type=MESH)
    for c in loads: c.wait()
    sent=[]
    f32=jnp.float32; bf=jnp.bfloat16
    def piece(sx,sz,j):
        cc=pl.ds(pl.multiple_of(j*CC,CC),CC)
        return cc,lax.dot_general(d_ref[2*sx+sz],w_s[cc,:],(((1,),(1,)),((),())),preferred_element_type=f32).reshape(2,half,CC)
    def compute_other(sx):
        def step(j,_):
            cc,p=piece(sx,o,j); po[sx,:,:,cc]=p.astype(bf); return 0
        lax.fori_loop(0,feat//CC,step,0)
    def compute_own(sx):
        def step(j,_):
            cc,p=piece(sx,z,j); pw[sx,:,:,cc]=p.astype(bf); return 0
        lax.fori_loop(0,SPLIT//CC,step,0)
        got(12+0,sx)
        def step2(j,_):
            cc,p=piece(sx,z,j)
            qq=pl.ds(pl.multiple_of(j*CC-SPLIT,CC),CC)
            pw[sx,:,:,cc]=(p+rq[sx,:,:,qq].astype(f32)).astype(bf); return 0
        lax.fori_loop(SPLIT//CC,feat//CC,step2,0)
    def copy(k,src,dst,dev):
        return pltpu.make_async_remote_copy(src_ref=src,dst_ref=dst,send_sem=send.at[k],recv_sem=recv.at[k],device_id=dev,device_id_type=MESH)
    def go(k,src,dst,dev):
        c=copy(k,src,dst,dev); c.start(); sent.append(c)
    qsem={}
    def got(k,sx=None):
        if k==12:
            copy(12+sx,rq.at[sx],rq.at[sx],to_z).wait_recv()
        elif k<6: copy(k,ro.at[k],ro.at[k],to_z).wait_recv()
        elif k<12: copy(k,rw.at[k-6],rw.at[k-6],to_z).wait_recv()
        else: copy(k,rp.at[k-16],rp.at[k-16],to_z).wait_recv()
    def zsend(sx):
        go(12+sx,po.at[sx,:,:,hi],rq.at[sx],to_z)
    W=1024
    def add(dst,terms,width):
        def step(j,_):
            cc=pl.ds(pl.multiple_of(j*CC,CC),CC)
            acc=terms[0][:,cc].astype(f32)
            for t in terms[1:]: acc=acc+t[:,cc].astype(f32)
            dst[:,cc]=acc.astype(bf); return 0
        lax.fori_loop(0,width//CC,step,0)
    compute_other(far)
    pl.semaphore_wait(bar,3)
    go(0,po.at[far,0,:,lo],ro.at[0],to_right); go(1,po.at[far,1,:,lo],ro.at[1],to_left); zsend(far)
    compute_other(right); go(2,po.at[right,1,:,lo],ro.at[2],to_right); zsend(right)
    compute_other(left); go(3,po.at[left,0,:,lo],ro.at[3],to_left); zsend(left)
    compute_other(x); zsend(x)
    got(0); add(po.at[right,0],[po.at[right,0],ro.at[0]],SPLIT); go(4,po.at[right,0,:,lo],ro.at[4],to_right)
    got(1); add(po.at[left,1],[po.at[left,1],ro.at[1]],SPLIT); go(5,po.at[left,1,:,lo],ro.at[5],to_left)
    compute_own(far)
    go(6,pw.at[far,0],rw.at[0],to_right); go(7,pw.at[far,1],rw.at[1],to_left)
    got(3); got(4); add(po.at[x,0],[po.at[x,0],ro.at[4],ro.at[3]],SPLIT); go(16,po.at[x,0,:,lo],rp.at[0],to_z)
    got(2); got(5); add(po.at[x,1],[po.at[x,1],ro.at[5],ro.at[2]],SPLIT); go(17,po.at[x,1,:,lo],rp.at[1],to_z)
    compute_own(right); go(8,pw.at[right,1],rw.at[2],to_right)
    compute_own(left); go(9,pw.at[left,0],rw.at[3],to_left)
    got(6); add(pw.at[right,0],[pw.at[right,0],rw.at[0]],feat); go(10,pw.at[right,0],rw.at[4],to_right)
    got(7); add(pw.at[left,1],[pw.at[left,1],rw.at[1]],feat); go(11,pw.at[left,1],rw.at[5],to_left)
    compute_own(x)
    def final(h,a,b):
        def low(j,_):
            cc=pl.ds(pl.multiple_of(j*CC,CC),CC)
            out_ref[h,:,cc]=(pw[x,h,:,cc].astype(f32)+rw[a,:,cc].astype(f32)+rw[b,:,cc].astype(f32)+rp[h,:,cc].astype(f32)).astype(bf); return 0
        def high(j,_):
            cc=pl.ds(pl.multiple_of(j*CC,CC),CC)
            out_ref[h,:,cc]=(pw[x,h,:,cc].astype(f32)+rw[a,:,cc].astype(f32)+rw[b,:,cc].astype(f32)).astype(bf); return 0
        lax.fori_loop(0,SPLIT//CC,low,0)
        lax.fori_loop(SPLIT//CC,feat//CC,high,0)
    got(9); got(10); got(16); final(0,4,3)
    got(8); got(11); got(17); final(1,5,2)
    for c in sent: c.wait_send()

def project_scatter(d,wq,wk,wv):
    seq,cols=d.shape; feat=wq.shape[0]; rows=seq//8; half=rows//2
    any_=pl.BlockSpec(memory_space=pl.ANY); vm=pl.BlockSpec(memory_space=pltpu.VMEM)
    bf=jnp.bfloat16
    out=pl.pallas_call(scatter_kernel,
        out_shape=jax.ShapeDtypeStruct((2,half,feat),bf),
        in_specs=[vm]+[any_]*3,out_specs=vm,
        scratch_shapes=[pltpu.VMEM((feat,cols),bf),pltpu.VMEM((4,2,half,feat),bf),pltpu.VMEM((4,2,half,feat),bf),
            pltpu.VMEM((6,half,SPLIT),bf),pltpu.VMEM((6,half,feat),bf),pltpu.VMEM((4,2,half,feat-SPLIT),bf),pltpu.VMEM((2,half,SPLIT),bf),
            pltpu.SemaphoreType.DMA((18,)),pltpu.SemaphoreType.DMA((18,)),pltpu.SemaphoreType.DMA((3,))],
        compiler_params=pltpu.CompilerParams(collective_id=2,has_side_effects=True,vmem_limit_bytes=60*2**20),name="project_scatter",
        cost_estimate=pl.CostEstimate(flops=2*seq*feat*cols,bytes_accessed=32*2**20,transcendentals=0),
    )(d.reshape(8,rows,cols),wq,wk,wv)
    return out.reshape(rows,feat)

STAGES = ((("c",), (2,)), (("zl", "zh"), (2, 2)), (("y",), (4,)), (("x",), (4,)))


def place(axes, sizes, index):
    where = {}
    for axis, size in zip(reversed(axes), reversed(sizes)):
        where[axis] = lax.rem(index, size)
        index = lax.div(index, size)
    return where


def total_kernel(part_ref, out_ref, b0, b1, b2, b3, send, recv):
    bufs = (b0, b1, b2, b3)
    bar = pltpu.get_barrier_semaphore()
    plan = []
    for axes, sizes in STAGES:
        n = 1
        me = jnp.int32(0)
        for axis, size in zip(axes, sizes):
            n *= size
            me = me * size + lax.axis_index(axis)
        others = [lax.rem(me + k, n) for k in range(1, n)]
        plan.append((n, me, others, [place(axes, sizes, other) for other in others]))
    count = 0
    for n, me, others, devices in plan:
        for device in devices:
            pl.semaphore_signal(bar, inc=1, device_id=device, device_id_type=MESH)
            count += 1
    value = part_ref[...]
    pl.semaphore_wait(bar, count)
    for stage, (n, me, others, devices) in enumerate(plan):
        buf = bufs[stage]
        buf[me] = value
        copies = []
        for k, device in enumerate(devices):
            copy = pltpu.make_async_remote_copy(
                src_ref=buf.at[me],
                dst_ref=buf.at[me],
                send_sem=send.at[stage, k],
                recv_sem=recv.at[stage, me],
                device_id=device,
                device_id_type=MESH,
            )
            copy.start()
            copies.append(copy)
        for k, other in enumerate(others):
            pltpu.make_async_remote_copy(
                src_ref=buf.at[other],
                dst_ref=buf.at[other],
                send_sem=send.at[stage, k],
                recv_sem=recv.at[stage, other],
                device_id=devices[k],
                device_id_type=MESH,
            ).wait_recv()
        value = buf[0]
        for k in range(1, n):
            value = value + buf[k]
        for copy in copies:
            copy.wait_send()
    out_ref[...] = value


def total_over_devices(part):
    vm = pl.BlockSpec(memory_space=pltpu.VMEM)
    shape = (part.shape[0] // 128, 128)
    out = pl.pallas_call(
        total_kernel,
        out_shape=jax.ShapeDtypeStruct(shape, jnp.float32),
        in_specs=[vm],
        out_specs=vm,
        scratch_shapes=[
            pltpu.VMEM((2,) + shape, jnp.float32),
            pltpu.VMEM((4,) + shape, jnp.float32),
            pltpu.VMEM((4,) + shape, jnp.float32),
            pltpu.VMEM((4,) + shape, jnp.float32),
            pltpu.SemaphoreType.DMA((4, 4)),
            pltpu.SemaphoreType.DMA((4, 4)),
        ],
        compiler_params=pltpu.CompilerParams(collective_id=3, has_side_effects=True),
        name="total",
        cost_estimate=pl.CostEstimate(flops=10**9, bytes_accessed=10**6, transcendentals=0),
    )(part.reshape(shape))
    return out.reshape(part.shape)


def rope_tables(segment_row):
    length = segment_row.shape[0]
    earlier = (segment_row[None, :] < segment_row[:, None]).astype(jnp.int32)
    offset = jnp.arange(length, dtype=jnp.int32) - jnp.sum(earlier, axis=1)
    half_dim = HD // 2
    inverse_freq = rope_base ** (-(jnp.arange(half_dim, dtype=jnp.float32) * 2.0 / HD))
    angle = offset.astype(jnp.float32)[:, None] * inverse_freq[None, :]
    cosine, sine = jnp.cos(angle), jnp.sin(angle)
    return jnp.concatenate([cosine, cosine], axis=1), jnp.concatenate([-sine, sine], axis=1)


def body(x_tokens, segment_ids, attended_grad, norm_gain, w_query, w_key, w_value):
    segment_row = segment_ids[0]
    as_float = x_tokens.astype(jnp.float32)
    inverse = lax.rsqrt(jnp.mean(as_float * as_float, axis=1, keepdims=True) + epsilon)
    own = (as_float * inverse * norm_gain).astype(jnp.bfloat16)
    qkv, normed = gather_project(own, w_query, w_key, w_value)
    cosine, sine = rope_tables(segment_row)
    attended, heads_d = attention(qkv, attended_grad, cosine, sine, segment_row)
    products = lax.dot_general(
        normed, heads_d, (((0,), (0,)), ((), ())), preferred_element_type=jnp.float32
    ).astype(jnp.bfloat16)
    heads_d, products = lax.optimization_barrier((heads_d, products))
    merged = lax.psum_scatter(products, DP, scatter_dimension=0, tiled=True).astype(jnp.float32)
    normed_d = project_scatter(heads_d, w_query, w_key, w_value).astype(jnp.float32)
    x_hat = x_tokens.astype(jnp.float32) * inverse
    scaled_d = normed_d * norm_gain
    input_grad = (
        inverse * (scaled_d - x_hat * jnp.mean(scaled_d * x_hat, axis=1, keepdims=True))
    ).astype(jnp.bfloat16)
    gain_grad = total_over_devices(jnp.sum(normed_d * x_hat, axis=0))
    query_cols, key_cols = w_query.shape[1], w_key.shape[1]
    return (
        attended,
        input_grad,
        gain_grad,
        merged[:, :query_cols],
        merged[:, query_cols : query_cols + key_cols],
        merged[:, query_cols + key_cols :],
    )


def solution(mesh):
    torus = Mesh(mesh.devices.reshape(4, 2, 2, 4, 2), DP_TP)
    return jax.shard_map(
        body,
        mesh=torus,
        in_specs=(
            P(DP_TP, None),
            P(DP, None),
            P(DP, TP),
            P(),
            P(None, TP),
            P(None, TP),
            P(None, TP),
        ),
        out_specs=(P(DP, TP), P(DP_TP, None), P(), P(DP, TP), P(DP, TP), P(DP, TP)),
        check_vma=False,
    )
```

```python
import jax
import jax.numpy as jnp
from jax import lax
from jax.experimental import pallas as pl
from jax.experimental.pallas import tpu as pltpu
from jax.sharding import Mesh
from jax.sharding import PartitionSpec as P

HD = 128
SPLIT = 4608
MESH = pl.DeviceIdType.MESH
TP = ("x", "zh")
DP = ("y", "zl", "c")
DP_TP = ("y", "zl", "c", "x", "zh")
epsilon = 1e-05
rope_base = 500000.0
def gather_kernel(n_ref, wq_ref, wk_ref, wv_ref, qkv_ref, full_ref, a_s, w_s, send, recv, local):
    x=lax.axis_index("x"); z=lax.axis_index("zh")
    right=lax.rem(x+1,4); left=lax.rem(x+3,4); far=lax.rem(x+2,4)
    to_right={"x":right}; to_left={"x":left}; to_z={"zh":1-z}
    half=a_s.shape[2]; rows=2*half
    lo=pl.ds(0,SPLIT); hi=pl.ds(SPLIT,a_s.shape[3]-SPLIT); every=pl.ds(0,a_s.shape[3])
    own=pltpu.make_async_copy(n_ref,a_s.at[2*x+z],local.at[0]); own.start()
    bar=pltpu.get_barrier_semaphore()
    for dev in (to_right,to_left,to_z):
        pl.semaphore_signal(bar,inc=1,device_id=dev,device_id_type=MESH)
    own.wait()
    pl.semaphore_wait(bar,3)
    wide=wq_ref.shape[1]; narrow=wk_ref.shape[1]
    loads=[pltpu.make_async_copy(wq_ref,w_s.at[:,pl.ds(0,wide)],local.at[1]),
           pltpu.make_async_copy(wk_ref,w_s.at[:,pl.ds(wide,narrow)],local.at[2]),
           pltpu.make_async_copy(wv_ref,w_s.at[:,pl.ds(wide+narrow,narrow)],local.at[3])]
    sent=[]
    def copy(k,sx,sz,h,cols,dev):
        ref=a_s.at[2*sx+sz,h,:,cols]
        return pltpu.make_async_remote_copy(src_ref=ref,dst_ref=ref,send_sem=send.at[k],recv_sem=recv.at[k],device_id=dev,device_id_type=MESH)
    def go(k,sx,sz,h,cols,dev):
        c=copy(k,sx,sz,h,cols,dev); c.start(); sent.append(c)
    def got(k,sx,sz,h,cols):
        copy(k,sx,sz,h,cols,to_z).wait_recv()
    o=1-z
    go(0,x,z,0,every,to_right); go(1,x,z,1,every,to_left)
    go(6,x,z,0,lo,to_z); go(7,x,z,1,lo,to_z)
    go(2,x,z,1,every,to_right); go(3,x,z,0,every,to_left)
    go(8,x,z,0,hi,to_z); go(9,x,z,1,hi,to_z)
    for c in loads: c.start()
    outs=[]
    def done(i,sx,sz):
        c=pltpu.make_async_copy(a_s.at[2*sx+sz],full_ref.at[2*sx+sz],local.at[4+i]); c.start(); outs.append(c)
    def project(slots):
        def one(i,_):
            s=slots(i)
            r=pl.ds(pl.multiple_of(s*rows,rows),rows)
            def part(j,_):
                kk=pl.ds(pl.multiple_of(j*KC,KC),KC)
                p=lax.dot_general(a_s[s,:,:,kk].reshape(rows,KC),w_s[kk,:],(((1,),(0,)),((),())),preferred_element_type=jnp.float32)
                qkv_ref[r,:]=jnp.where(j==0,p,qkv_ref[r,:]+p)
                return 0
            lax.fori_loop(0,a_s.shape[3]//KC,part,0)
            return 0
        return one
    KC=2048
    def run(n,f): lax.fori_loop(0,n,project(f),0)
    done(0,x,z)
    for c in loads: c.wait()
    run(1,lambda i: 2*x+z)
    got(0,left,z,0,every); go(4,left,z,0,every,to_right); go(10,left,z,0,hi,to_z)
    got(1,right,z,1,every); go(5,right,z,1,every,to_left); go(11,right,z,1,hi,to_z)
    got(6,x,o,0,lo); go(12,x,o,0,lo,to_right); got(7,x,o,1,lo); go(13,x,o,1,lo,to_left)
    go(14,x,o,1,lo,to_right); go(15,x,o,0,lo,to_left)
    got(2,left,z,1,every); go(16,left,z,1,hi,to_z)
    got(3,right,z,0,every); go(17,right,z,0,hi,to_z)
    done(1,left,z); done(2,right,z)
    got(8,x,o,0,hi); got(9,x,o,1,hi); done(3,x,o)
    run(2,lambda i: 2*lax.rem(x+1+2*i,4)+z)
    got(4,far,z,0,every); go(18,far,z,0,hi,to_z)
    got(5,far,z,1,every); go(19,far,z,1,hi,to_z)
    done(4,far,z)
    run(1,lambda i: 2*x+o)
    got(12,left,o,0,lo); go(20,left,o,0,lo,to_right)
    got(13,right,o,1,lo); go(21,right,o,1,lo,to_left)
    run(1,lambda i: 2*far+z)
    got(10,left,o,0,hi); got(11,right,o,1,hi)
    got(14,left,o,1,lo); got(16,left,o,1,hi); done(5,left,o)
    got(15,right,o,0,lo); got(17,right,o,0,hi); done(6,right,o)
    run(2,lambda i: 2*lax.rem(x+1+2*i,4)+o)
    got(20,far,o,0,lo); got(21,far,o,1,lo); got(18,far,o,0,hi); got(19,far,o,1,hi); done(7,far,o)
    run(1,lambda i: 2*far+o)
    for c in sent: c.wait_send()
    for c in outs: c.wait()

def gather_project(normed,wq,wk,wv):
    rows,feat=normed.shape
    cols=wq.shape[1]+2*wk.shape[1]
    any_=pl.BlockSpec(memory_space=pl.ANY); vm=pl.BlockSpec(memory_space=pltpu.VMEM)
    qkv,full=pl.pallas_call(gather_kernel,
        out_shape=(jax.ShapeDtypeStruct((8*rows,cols),jnp.float32),jax.ShapeDtypeStruct((8,2,rows//2,feat),jnp.bfloat16)),
        in_specs=[any_]*4,out_specs=(vm,any_),
        scratch_shapes=[pltpu.VMEM((8,2,rows//2,feat),jnp.bfloat16),pltpu.VMEM((feat,cols),jnp.bfloat16),
            pltpu.SemaphoreType.DMA((22,)),pltpu.SemaphoreType.DMA((22,)),pltpu.SemaphoreType.DMA((12,))],
        compiler_params=pltpu.CompilerParams(collective_id=1,has_side_effects=True,vmem_limit_bytes=60*2**20),name="gather_project",
        cost_estimate=pl.CostEstimate(flops=2*8*rows*feat*cols,bytes_accessed=48*2**20,transcendentals=0),
    )(normed.reshape(2,rows//2,feat),wq,wk,wv)
    return qkv,full.reshape(8*rows,feat)
BQ=256
def _nt(a,b): return lax.dot_general(a,b,(((1,),(1,)),((),())),preferred_element_type=jnp.float32)
def _tn(a,b): return lax.dot_general(a,b,(((0,),(0,)),((),())),preferred_element_type=jnp.float32)
def _nn(a,b): return lax.dot_general(a,b,(((1,),(0,)),((),())),preferred_element_type=jnp.float32)

def attention_kernel(qkv_ref, go_ref, cos_ref, sin_ref, segr_ref, segc_ref, att_ref, d_ref, q_s, k_s, v_s, dk_s, dv_s):
    seq=qkv_ref.shape[0]; heads=go_ref.shape[1]//HD; width=heads*HD
    scale=float(HD)**-0.5
    def rope(u,c,s): return u*c+pltpu.roll(u,HD//2,1)*s
    nb=seq//BQ
    for b in range(nb):
        r=slice(b*BQ,(b+1)*BQ)
        c=cos_ref[r,:]; s=sin_ref[r,:]
        for h in range(heads):
            q_s[r,h*HD:(h+1)*HD]=rope(qkv_ref[r,h*HD:(h+1)*HD],c,s).astype(jnp.bfloat16)
        k_s[r,:]=rope(qkv_ref[r,width:width+HD],c,s).astype(jnp.bfloat16)
        v_s[r,:]=qkv_ref[r,width+HD:width+2*HD].astype(jnp.bfloat16)
    dk_s[...]=jnp.zeros_like(dk_s)
    dv_s[...]=jnp.zeros_like(dv_s)
    for b in range(nb):
        r=slice(b*BQ,(b+1)*BQ)
        lo=max(0,(b*BQ-511)//BQ*BQ); hi=(b+1)*BQ
        kr=slice(lo,hi)
        rows=lax.broadcasted_iota(jnp.int32,(BQ,hi-lo),0)+b*BQ
        cols=lax.broadcasted_iota(jnp.int32,(BQ,hi-lo),1)+lo
        mask=(cols<=rows)&(segr_ref[0:1,kr]==segc_ref[r,0:1])
        def head(h,_):
            hs=pl.ds(pl.multiple_of(h*HD,HD),HD)
            q=q_s[r,hs]; go=go_ref[r,hs]
            k=k_s[kr,:]; v=v_s[kr,:]
            sc=jnp.where(mask,_nt(q,k)*scale,-1e30)
            m=jnp.max(sc,axis=1,keepdims=True)
            e=jnp.exp(sc-m)
            p=e*(1.0/jnp.sum(e,axis=1,keepdims=True))
            w=p.astype(jnp.bfloat16)
            o=_nn(w,v).astype(jnp.bfloat16)
            att_ref[r,hs]=o
            delta=jnp.sum(go.astype(jnp.float32)*o.astype(jnp.float32),axis=1,keepdims=True)
            dv_s[kr,:]+=_tn(w,go)
            dp=_nt(go,v)
            ds=(p*(dp-delta)*scale).astype(jnp.bfloat16)
            dq=_nn(ds,k)
            d_ref[r,hs]=rope(dq,cos_ref[r,:],-sin_ref[r,:]).astype(jnp.bfloat16)
            dk_s[kr,:]+=_tn(ds,q)
            return 0
        lax.fori_loop(0,heads,head,0,unroll=True)
    d_ref[:,width:width+HD]=rope(dk_s[...],cos_ref[...],-sin_ref[...]).astype(jnp.bfloat16)
    d_ref[:,width+HD:width+2*HD]=dv_s[...].astype(jnp.bfloat16)

def attention(qkv,go,cos,sin,segs):
    seq=qkv.shape[0]
    vm=pl.BlockSpec(memory_space=pltpu.VMEM)
    return pl.pallas_call(attention_kernel,
        out_shape=(jax.ShapeDtypeStruct(go.shape,jnp.bfloat16),jax.ShapeDtypeStruct(qkv.shape,jnp.bfloat16)),
        in_specs=[vm]*6,out_specs=(vm,vm),
        scratch_shapes=[pltpu.VMEM(go.shape,jnp.bfloat16),pltpu.VMEM((seq,HD),jnp.bfloat16),pltpu.VMEM((seq,HD),jnp.bfloat16),pltpu.VMEM((seq,HD),jnp.float32),pltpu.VMEM((seq,HD),jnp.float32)],
        compiler_params=pltpu.CompilerParams(vmem_limit_bytes=60*2**20),name="attention",
        cost_estimate=pl.CostEstimate(flops=12*go.shape[1]*seq*seq//2,bytes_accessed=12*2**20,transcendentals=0),
    )(qkv,go,cos,sin,segs.reshape(1,seq),segs.reshape(seq,1))
CC=512
def scatter_kernel(d_ref, wq_ref, wk_ref, wv_ref, out_ref, w_s, po, pw, ro, rw, rq, rp, send, recv, local):
    x=lax.axis_index("x"); z=lax.axis_index("zh"); o=1-z
    right=lax.rem(x+1,4); left=lax.rem(x+3,4); far=lax.rem(x+2,4)
    to_right={"x":right}; to_left={"x":left}; to_z={"zh":o}
    feat=po.shape[3]; half=po.shape[2]; rows=2*half
    lo=pl.ds(0,SPLIT); hi=pl.ds(SPLIT,feat-SPLIT); every=pl.ds(0,feat)
    wide=wq_ref.shape[1]; narrow=wk_ref.shape[1]
    loads=[pltpu.make_async_copy(wq_ref,w_s.at[:,pl.ds(0,wide)],local.at[0]),
           pltpu.make_async_copy(wk_ref,w_s.at[:,pl.ds(wide,narrow)],local.at[1]),
           pltpu.make_async_copy(wv_ref,w_s.at[:,pl.ds(wide+narrow,narrow)],local.at[2])]
    for c in loads: c.start()
    bar=pltpu.get_barrier_semaphore()
    for dev in (to_right,to_left,to_z):
        pl.semaphore_signal(bar,inc=1,device_id=dev,device_id_type=MESH)
    for c in loads: c.wait()
    sent=[]
    f32=jnp.float32; bf=jnp.bfloat16
    def piece(sx,sz,j):
        cc=pl.ds(pl.multiple_of(j*CC,CC),CC)
        return cc,lax.dot_general(d_ref[2*sx+sz],w_s[cc,:],(((1,),(1,)),((),())),preferred_element_type=f32).reshape(2,half,CC)
    def compute_other(sx):
        def step(j,_):
            cc,p=piece(sx,o,j); po[sx,:,:,cc]=p.astype(bf); return 0
        lax.fori_loop(0,feat//CC,step,0)
    def compute_own(sx):
        def step(j,_):
            cc,p=piece(sx,z,j); pw[sx,:,:,cc]=p.astype(bf); return 0
        lax.fori_loop(0,SPLIT//CC,step,0)
        got(12+0,sx)
        def step2(j,_):
            cc,p=piece(sx,z,j)
            qq=pl.ds(pl.multiple_of(j*CC-SPLIT,CC),CC)
            pw[sx,:,:,cc]=(p+rq[sx,:,:,qq].astype(f32)).astype(bf); return 0
        lax.fori_loop(SPLIT//CC,feat//CC,step2,0)
    def copy(k,src,dst,dev):
        return pltpu.make_async_remote_copy(src_ref=src,dst_ref=dst,send_sem=send.at[k],recv_sem=recv.at[k],device_id=dev,device_id_type=MESH)
    def go(k,src,dst,dev):
        c=copy(k,src,dst,dev); c.start(); sent.append(c)
    qsem={}
    def got(k,sx=None):
        if k==12:
            copy(12+sx,rq.at[sx],rq.at[sx],to_z).wait_recv()
        elif k<6: copy(k,ro.at[k],ro.at[k],to_z).wait_recv()
        elif k<12: copy(k,rw.at[k-6],rw.at[k-6],to_z).wait_recv()
        else: copy(k,rp.at[k-16],rp.at[k-16],to_z).wait_recv()
    def zsend(sx):
        go(12+sx,po.at[sx,:,:,hi],rq.at[sx],to_z)
    W=1024
    def add(dst,terms,width):
        def step(j,_):
            cc=pl.ds(pl.multiple_of(j*CC,CC),CC)
            acc=terms[0][:,cc].astype(f32)
            for t in terms[1:]: acc=acc+t[:,cc].astype(f32)
            dst[:,cc]=acc.astype(bf); return 0
        lax.fori_loop(0,width//CC,step,0)
    compute_other(far)
    pl.semaphore_wait(bar,3)
    go(0,po.at[far,0,:,lo],ro.at[0],to_right); go(1,po.at[far,1,:,lo],ro.at[1],to_left); zsend(far)
    compute_other(right); go(2,po.at[right,1,:,lo],ro.at[2],to_right); zsend(right)
    compute_other(left); go(3,po.at[left,0,:,lo],ro.at[3],to_left); zsend(left)
    compute_other(x); zsend(x)
    got(0); add(po.at[right,0],[po.at[right,0],ro.at[0]],SPLIT); go(4,po.at[right,0,:,lo],ro.at[4],to_right)
    got(1); add(po.at[left,1],[po.at[left,1],ro.at[1]],SPLIT); go(5,po.at[left,1,:,lo],ro.at[5],to_left)
    compute_own(far)
    go(6,pw.at[far,0],rw.at[0],to_right); go(7,pw.at[far,1],rw.at[1],to_left)
    got(3); got(4); add(po.at[x,0],[po.at[x,0],ro.at[4],ro.at[3]],SPLIT); go(16,po.at[x,0,:,lo],rp.at[0],to_z)
    got(2); got(5); add(po.at[x,1],[po.at[x,1],ro.at[5],ro.at[2]],SPLIT); go(17,po.at[x,1,:,lo],rp.at[1],to_z)
    compute_own(right); go(8,pw.at[right,1],rw.at[2],to_right)
    compute_own(left); go(9,pw.at[left,0],rw.at[3],to_left)
    got(6); add(pw.at[right,0],[pw.at[right,0],rw.at[0]],feat); go(10,pw.at[right,0],rw.at[4],to_right)
    got(7); add(pw.at[left,1],[pw.at[left,1],rw.at[1]],feat); go(11,pw.at[left,1],rw.at[5],to_left)
    compute_own(x)
    def final(h,a,b):
        def low(j,_):
            cc=pl.ds(pl.multiple_of(j*CC,CC),CC)
            out_ref[h,:,cc]=(pw[x,h,:,cc].astype(f32)+rw[a,:,cc].astype(f32)+rw[b,:,cc].astype(f32)+rp[h,:,cc].astype(f32)).astype(bf); return 0
        def high(j,_):
            cc=pl.ds(pl.multiple_of(j*CC,CC),CC)
            out_ref[h,:,cc]=(pw[x,h,:,cc].astype(f32)+rw[a,:,cc].astype(f32)+rw[b,:,cc].astype(f32)).astype(bf); return 0
        lax.fori_loop(0,SPLIT//CC,low,0)
        lax.fori_loop(SPLIT//CC,feat//CC,high,0)
    got(9); got(10); got(16); final(0,4,3)
    got(8); got(11); got(17); final(1,5,2)
    for c in sent: c.wait_send()

def project_scatter(d,wq,wk,wv):
    seq,cols=d.shape; feat=wq.shape[0]; rows=seq//8; half=rows//2
    any_=pl.BlockSpec(memory_space=pl.ANY); vm=pl.BlockSpec(memory_space=pltpu.VMEM)
    bf=jnp.bfloat16
    out=pl.pallas_call(scatter_kernel,
        out_shape=jax.ShapeDtypeStruct((2,half,feat),bf),
        in_specs=[vm]+[any_]*3,out_specs=vm,
        scratch_shapes=[pltpu.VMEM((feat,cols),bf),pltpu.VMEM((4,2,half,feat),bf),pltpu.VMEM((4,2,half,feat),bf),
            pltpu.VMEM((6,half,SPLIT),bf),pltpu.VMEM((6,half,feat),bf),pltpu.VMEM((4,2,half,feat-SPLIT),bf),pltpu.VMEM((2,half,SPLIT),bf),
            pltpu.SemaphoreType.DMA((18,)),pltpu.SemaphoreType.DMA((18,)),pltpu.SemaphoreType.DMA((3,))],
        compiler_params=pltpu.CompilerParams(collective_id=2,has_side_effects=True,vmem_limit_bytes=60*2**20),name="project_scatter",
        cost_estimate=pl.CostEstimate(flops=2*seq*feat*cols,bytes_accessed=32*2**20,transcendentals=0),
    )(d.reshape(8,rows,cols),wq,wk,wv)
    return out.reshape(rows,feat)

STAGES = ((("c",), (2,)), (("zl", "zh"), (2, 2)), (("y",), (4,)), (("x",), (4,)))


def place(axes, sizes, index):
    where = {}
    for axis, size in zip(reversed(axes), reversed(sizes)):
        where[axis] = lax.rem(index, size)
        index = lax.div(index, size)
    return where


def total_kernel(part_ref, out_ref, b0, b1, b2, b3, send, recv):
    bufs = (b0, b1, b2, b3)
    bar = pltpu.get_barrier_semaphore()
    plan = []
    for axes, sizes in STAGES:
        n = 1
        me = jnp.int32(0)
        for axis, size in zip(axes, sizes):
            n *= size
            me = me * size + lax.axis_index(axis)
        others = [lax.rem(me + k, n) for k in range(1, n)]
        plan.append((n, me, others, [place(axes, sizes, other) for other in others]))
    count = 0
    for n, me, others, devices in plan:
        for device in devices:
            pl.semaphore_signal(bar, inc=1, device_id=device, device_id_type=MESH)
            count += 1
    value = part_ref[...]
    pl.semaphore_wait(bar, count)
    for stage, (n, me, others, devices) in enumerate(plan):
        buf = bufs[stage]
        buf[me] = value
        copies = []
        for k, device in enumerate(devices):
            copy = pltpu.make_async_remote_copy(
                src_ref=buf.at[me],
                dst_ref=buf.at[me],
                send_sem=send.at[stage, k],
                recv_sem=recv.at[stage, me],
                device_id=device,
                device_id_type=MESH,
            )
            copy.start()
            copies.append(copy)
        for k, other in enumerate(others):
            pltpu.make_async_remote_copy(
                src_ref=buf.at[other],
                dst_ref=buf.at[other],
                send_sem=send.at[stage, k],
                recv_sem=recv.at[stage, other],
                device_id=devices[k],
                device_id_type=MESH,
            ).wait_recv()
        value = buf[0]
        for k in range(1, n):
            value = value + buf[k]
        for copy in copies:
            copy.wait_send()
    out_ref[...] = value


def total_over_devices(part):
    vm = pl.BlockSpec(memory_space=pltpu.VMEM)
    shape = (part.shape[0] // 128, 128)
    out = pl.pallas_call(
        total_kernel,
        out_shape=jax.ShapeDtypeStruct(shape, jnp.float32),
        in_specs=[vm],
        out_specs=vm,
        scratch_shapes=[
            pltpu.VMEM((2,) + shape, jnp.float32),
            pltpu.VMEM((4,) + shape, jnp.float32),
            pltpu.VMEM((4,) + shape, jnp.float32),
            pltpu.VMEM((4,) + shape, jnp.float32),
            pltpu.SemaphoreType.DMA((4, 4)),
            pltpu.SemaphoreType.DMA((4, 4)),
        ],
        compiler_params=pltpu.CompilerParams(collective_id=3, has_side_effects=True),
        name="total",
        cost_estimate=pl.CostEstimate(flops=10**9, bytes_accessed=10**6, transcendentals=0),
    )(part.reshape(shape))
    return out.reshape(part.shape)


def gradient_kernel(n_ref, d_ref, out_ref, n_s, dt_s, mine, theirs, send, recv, local):
    c = lax.axis_index("c")
    count = out_ref.shape[0]
    width = out_ref.shape[2]

    def load(i):
        block = jnp.where(i < count, 2 * i + 1 - c, 2 * (i - count) + c)
        cols = pl.ds(pl.multiple_of(block * width, width), width)
        return pltpu.make_async_copy(n_ref.at[:, cols], n_s.at[i], local.at[i])

    def start(i, _):
        load(i).start()
        return 0

    lax.fori_loop(0, 2 * count, start, 0)
    bar = pltpu.get_barrier_semaphore()
    pl.semaphore_signal(bar, inc=1, device_id={"c": 1 - c}, device_id_type=MESH)
    dt_s[...] = d_ref[...].T
    pl.semaphore_wait(bar, 1)

    def copy(i):
        return pltpu.make_async_remote_copy(
            src_ref=mine.at[i],
            dst_ref=theirs.at[i],
            send_sem=send.at[i],
            recv_sem=recv.at[i],
            device_id={"c": 1 - c},
            device_id_type=MESH,
        )

    def product(i):
        load(i).wait()
        return jnp.dot(dt_s[...], n_s[i], preferred_element_type=jnp.float32)

    def first(i, _):
        mine[i] = product(i).astype(jnp.bfloat16)
        copy(i).start()
        return 0

    def second(i, _):
        part = product(i + count)
        copy(i).wait_recv()
        out_ref[i] = (part + theirs[i].astype(jnp.float32)).astype(jnp.bfloat16)
        return 0

    def last(i, _):
        copy(i).wait_send()
        return 0

    lax.fori_loop(0, count, first, 0)
    lax.fori_loop(0, count, second, 0)
    lax.fori_loop(0, count, last, 0)


def pair_gradient(normed, heads_d):
    seq, feat = normed.shape
    cols = heads_d.shape[1]
    count, width = 8, feat // 16
    vm = pl.BlockSpec(memory_space=pltpu.VMEM)
    bf = jnp.bfloat16
    return pl.pallas_call(
        gradient_kernel,
        out_shape=jax.ShapeDtypeStruct((count, cols, width), bf),
        in_specs=[pl.BlockSpec(memory_space=pl.ANY), vm],
        out_specs=vm,
        scratch_shapes=[
            pltpu.VMEM((2 * count, seq, width), bf),
            pltpu.VMEM((cols, seq), bf),
            pltpu.VMEM((count, cols, width), bf),
            pltpu.VMEM((count, cols, width), bf),
            pltpu.SemaphoreType.DMA((count,)),
            pltpu.SemaphoreType.DMA((count,)),
            pltpu.SemaphoreType.DMA((2 * count,)),
        ],
        compiler_params=pltpu.CompilerParams(
            collective_id=4, has_side_effects=True, vmem_limit_bytes=60 * 2**20
        ),
        name="pair_gradient",
        cost_estimate=pl.CostEstimate(
            flops=2 * seq * feat * cols, bytes_accessed=32 * 2**20, transcendentals=0
        ),
    )(normed, heads_d)


def rope_tables(segment_row):
    length = segment_row.shape[0]
    earlier = (segment_row[None, :] < segment_row[:, None]).astype(jnp.int32)
    offset = jnp.arange(length, dtype=jnp.int32) - jnp.sum(earlier, axis=1)
    half_dim = HD // 2
    inverse_freq = rope_base ** (-(jnp.arange(half_dim, dtype=jnp.float32) * 2.0 / HD))
    angle = offset.astype(jnp.float32)[:, None] * inverse_freq[None, :]
    cosine, sine = jnp.cos(angle), jnp.sin(angle)
    return jnp.concatenate([cosine, cosine], axis=1), jnp.concatenate([-sine, sine], axis=1)


def body(x_tokens, segment_ids, attended_grad, norm_gain, w_query, w_key, w_value):
    segment_row = segment_ids[0]
    as_float = x_tokens.astype(jnp.float32)
    inverse = lax.rsqrt(jnp.mean(as_float * as_float, axis=1, keepdims=True) + epsilon)
    own = (as_float * inverse * norm_gain).astype(jnp.bfloat16)
    qkv, normed = gather_project(own, w_query, w_key, w_value)
    cosine, sine = rope_tables(segment_row)
    attended, heads_d = attention(qkv, attended_grad, cosine, sine, segment_row)
    products = pair_gradient(normed, heads_d)
    heads_d, products = lax.optimization_barrier((heads_d, products))
    merged = lax.psum_scatter(products, "y", scatter_dimension=0, tiled=True)
    normed_d = project_scatter(heads_d, w_query, w_key, w_value)
    merged, normed_d = lax.optimization_barrier((merged, normed_d))
    merged = lax.psum_scatter(merged, "zl", scatter_dimension=0, tiled=True)
    merged = merged[0].T.astype(jnp.float32)
    normed_d = normed_d.astype(jnp.float32)
    x_hat = x_tokens.astype(jnp.float32) * inverse
    scaled_d = normed_d * norm_gain
    input_grad = (
        inverse * (scaled_d - x_hat * jnp.mean(scaled_d * x_hat, axis=1, keepdims=True))
    ).astype(jnp.bfloat16)
    gain_grad = total_over_devices(jnp.sum(normed_d * x_hat, axis=0))
    query_cols, key_cols = w_query.shape[1], w_key.shape[1]
    return (
        attended,
        input_grad,
        gain_grad,
        merged[:, :query_cols],
        merged[:, query_cols : query_cols + key_cols],
        merged[:, query_cols + key_cols :],
    )


def solution(mesh):
    torus = Mesh(mesh.devices.reshape(4, 2, 2, 4, 2), DP_TP)
    return jax.shard_map(
        body,
        mesh=torus,
        in_specs=(
            P(DP_TP, None),
            P(DP, None),
            P(DP, TP),
            P(),
            P(None, TP),
            P(None, TP),
            P(None, TP),
        ),
        out_specs=(P(DP, TP), P(DP_TP, None), P(), P(DP, TP), P(DP, TP), P(DP, TP)),
        check_vma=False,
    )
```

```python
import jax
import jax.numpy as jnp
from jax import lax
from jax.experimental import pallas as pl
from jax.experimental.pallas import tpu as pltpu
from jax.sharding import Mesh
from jax.sharding import PartitionSpec as P

HD = 128
SPLIT = 4608
MESH = pl.DeviceIdType.MESH
TP = ("x", "zh")
DP = ("y", "zl", "c")
DP_TP = ("y", "zl", "c", "x", "zh")
epsilon = 1e-05
rope_base = 500000.0
def gather_kernel(n_ref, wq_ref, wk_ref, wv_ref, qkv_ref, full_ref, a_s, w_s, send, recv, local):
    x=lax.axis_index("x"); z=lax.axis_index("zh")
    right=lax.rem(x+1,4); left=lax.rem(x+3,4); far=lax.rem(x+2,4)
    to_right={"x":right}; to_left={"x":left}; to_z={"zh":1-z}
    half=a_s.shape[2]; rows=2*half
    lo=pl.ds(0,SPLIT); hi=pl.ds(SPLIT,a_s.shape[3]-SPLIT); every=pl.ds(0,a_s.shape[3])
    own=pltpu.make_async_copy(n_ref,a_s.at[2*x+z],local.at[0]); own.start()
    bar=pltpu.get_barrier_semaphore()
    for dev in (to_right,to_left,to_z):
        pl.semaphore_signal(bar,inc=1,device_id=dev,device_id_type=MESH)
    own.wait()
    pl.semaphore_wait(bar,3)
    wide=wq_ref.shape[1]; narrow=wk_ref.shape[1]
    loads=[pltpu.make_async_copy(wq_ref,w_s.at[:,pl.ds(0,wide)],local.at[1]),
           pltpu.make_async_copy(wk_ref,w_s.at[:,pl.ds(wide,narrow)],local.at[2]),
           pltpu.make_async_copy(wv_ref,w_s.at[:,pl.ds(wide+narrow,narrow)],local.at[3])]
    sent=[]
    def copy(k,sx,sz,h,cols,dev):
        ref=a_s.at[2*sx+sz,h,:,cols]
        return pltpu.make_async_remote_copy(src_ref=ref,dst_ref=ref,send_sem=send.at[k],recv_sem=recv.at[k],device_id=dev,device_id_type=MESH)
    def go(k,sx,sz,h,cols,dev):
        c=copy(k,sx,sz,h,cols,dev); c.start(); sent.append(c)
    def got(k,sx,sz,h,cols):
        copy(k,sx,sz,h,cols,to_z).wait_recv()
    o=1-z
    go(0,x,z,0,every,to_right); go(1,x,z,1,every,to_left)
    go(6,x,z,0,lo,to_z); go(7,x,z,1,lo,to_z)
    go(2,x,z,1,every,to_right); go(3,x,z,0,every,to_left)
    go(8,x,z,0,hi,to_z); go(9,x,z,1,hi,to_z)
    for c in loads: c.start()
    outs=[]
    def done(i,sx,sz):
        c=pltpu.make_async_copy(a_s.at[2*sx+sz],full_ref.at[2*sx+sz],local.at[4+i]); c.start(); outs.append(c)
    def project(slots):
        def one(i,_):
            s=slots(i)
            r=pl.ds(pl.multiple_of(s*rows,rows),rows)
            def part(j,_):
                kk=pl.ds(pl.multiple_of(j*KC,KC),KC)
                p=lax.dot_general(a_s[s,:,:,kk].reshape(rows,KC),w_s[kk,:],(((1,),(0,)),((),())),preferred_element_type=jnp.float32)
                qkv_ref[r,:]=jnp.where(j==0,p,qkv_ref[r,:]+p)
                return 0
            lax.fori_loop(0,a_s.shape[3]//KC,part,0)
            return 0
        return one
    KC=2048
    def run(n,f): lax.fori_loop(0,n,project(f),0)
    done(0,x,z)
    for c in loads: c.wait()
    run(1,lambda i: 2*x+z)
    got(0,left,z,0,every); go(4,left,z,0,every,to_right); go(10,left,z,0,hi,to_z)
    got(1,right,z,1,every); go(5,right,z,1,every,to_left); go(11,right,z,1,hi,to_z)
    got(6,x,o,0,lo); go(12,x,o,0,lo,to_right); got(7,x,o,1,lo); go(13,x,o,1,lo,to_left)
    go(14,x,o,1,lo,to_right); go(15,x,o,0,lo,to_left)
    got(2,left,z,1,every); go(16,left,z,1,hi,to_z)
    got(3,right,z,0,every); go(17,right,z,0,hi,to_z)
    done(1,left,z); done(2,right,z)
    got(8,x,o,0,hi); got(9,x,o,1,hi); done(3,x,o)
    run(2,lambda i: 2*lax.rem(x+1+2*i,4)+z)
    got(4,far,z,0,every); go(18,far,z,0,hi,to_z)
    got(5,far,z,1,every); go(19,far,z,1,hi,to_z)
    done(4,far,z)
    run(1,lambda i: 2*x+o)
    got(12,left,o,0,lo); go(20,left,o,0,lo,to_right)
    got(13,right,o,1,lo); go(21,right,o,1,lo,to_left)
    run(1,lambda i: 2*far+z)
    got(10,left,o,0,hi); got(11,right,o,1,hi)
    got(14,left,o,1,lo); got(16,left,o,1,hi); done(5,left,o)
    got(15,right,o,0,lo); got(17,right,o,0,hi); done(6,right,o)
    run(2,lambda i: 2*lax.rem(x+1+2*i,4)+o)
    got(20,far,o,0,lo); got(21,far,o,1,lo); got(18,far,o,0,hi); got(19,far,o,1,hi); done(7,far,o)
    run(1,lambda i: 2*far+o)
    for c in sent: c.wait_send()
    for c in outs: c.wait()

def gather_project(normed,wq,wk,wv):
    rows,feat=normed.shape
    cols=wq.shape[1]+2*wk.shape[1]
    any_=pl.BlockSpec(memory_space=pl.ANY); vm=pl.BlockSpec(memory_space=pltpu.VMEM)
    qkv,full=pl.pallas_call(gather_kernel,
        out_shape=(jax.ShapeDtypeStruct((8*rows,cols),jnp.float32),jax.ShapeDtypeStruct((8,2,rows//2,feat),jnp.bfloat16)),
        in_specs=[any_]*4,out_specs=(vm,any_),
        scratch_shapes=[pltpu.VMEM((8,2,rows//2,feat),jnp.bfloat16),pltpu.VMEM((feat,cols),jnp.bfloat16),
            pltpu.SemaphoreType.DMA((22,)),pltpu.SemaphoreType.DMA((22,)),pltpu.SemaphoreType.DMA((12,))],
        compiler_params=pltpu.CompilerParams(collective_id=1,has_side_effects=True,vmem_limit_bytes=60*2**20),name="gather_project",
        cost_estimate=pl.CostEstimate(flops=2*8*rows*feat*cols,bytes_accessed=48*2**20,transcendentals=0),
    )(normed.reshape(2,rows//2,feat),wq,wk,wv)
    return qkv,full.reshape(8*rows,feat)
BQ=256
def _nt(a,b): return lax.dot_general(a,b,(((1,),(1,)),((),())),preferred_element_type=jnp.float32)
def _tn(a,b): return lax.dot_general(a,b,(((0,),(0,)),((),())),preferred_element_type=jnp.float32)
def _nn(a,b): return lax.dot_general(a,b,(((1,),(0,)),((),())),preferred_element_type=jnp.float32)

def attention_kernel(qkv_ref, go_ref, cos_ref, sin_ref, segr_ref, segc_ref, att_ref, d_ref, q_s, k_s, v_s, dk_s, dv_s):
    seq=qkv_ref.shape[0]; heads=go_ref.shape[1]//HD; width=heads*HD
    scale=float(HD)**-0.5
    def rope(u,c,s): return u*c+pltpu.roll(u,HD//2,1)*s
    nb=seq//BQ
    for b in range(nb):
        r=slice(b*BQ,(b+1)*BQ)
        c=cos_ref[r,:]; s=sin_ref[r,:]
        for h in range(heads):
            q_s[r,h*HD:(h+1)*HD]=rope(qkv_ref[r,h*HD:(h+1)*HD],c,s).astype(jnp.bfloat16)
        k_s[r,:]=rope(qkv_ref[r,width:width+HD],c,s).astype(jnp.bfloat16)
        v_s[r,:]=qkv_ref[r,width+HD:width+2*HD].astype(jnp.bfloat16)
    dk_s[...]=jnp.zeros_like(dk_s)
    dv_s[...]=jnp.zeros_like(dv_s)
    for b in range(nb):
        r=slice(b*BQ,(b+1)*BQ)
        lo=max(0,(b*BQ-511)//BQ*BQ); hi=(b+1)*BQ
        kr=slice(lo,hi)
        rows=lax.broadcasted_iota(jnp.int32,(BQ,hi-lo),0)+b*BQ
        cols=lax.broadcasted_iota(jnp.int32,(BQ,hi-lo),1)+lo
        mask=(cols<=rows)&(segr_ref[0:1,kr]==segc_ref[r,0:1])
        def head(h,_):
            hs=pl.ds(pl.multiple_of(h*HD,HD),HD)
            q=q_s[r,hs]; go=go_ref[r,hs]
            k=k_s[kr,:]; v=v_s[kr,:]
            sc=jnp.where(mask,_nt(q,k)*scale,-1e30)
            m=jnp.max(sc,axis=1,keepdims=True)
            e=jnp.exp(sc-m)
            p=e*(1.0/jnp.sum(e,axis=1,keepdims=True))
            w=p.astype(jnp.bfloat16)
            o=_nn(w,v).astype(jnp.bfloat16)
            att_ref[r,hs]=o
            delta=jnp.sum(go.astype(jnp.float32)*o.astype(jnp.float32),axis=1,keepdims=True)
            dv_s[kr,:]+=_tn(w,go)
            dp=_nt(go,v)
            ds=(p*(dp-delta)*scale).astype(jnp.bfloat16)
            dq=_nn(ds,k)
            d_ref[r,hs]=rope(dq,cos_ref[r,:],-sin_ref[r,:]).astype(jnp.bfloat16)
            dk_s[kr,:]+=_tn(ds,q)
            return 0
        lax.fori_loop(0,heads,head,0,unroll=True)
    d_ref[:,width:width+HD]=rope(dk_s[...],cos_ref[...],-sin_ref[...]).astype(jnp.bfloat16)
    d_ref[:,width+HD:width+2*HD]=dv_s[...].astype(jnp.bfloat16)

def attention(qkv,go,cos,sin,segs):
    seq=qkv.shape[0]
    vm=pl.BlockSpec(memory_space=pltpu.VMEM)
    return pl.pallas_call(attention_kernel,
        out_shape=(jax.ShapeDtypeStruct(go.shape,jnp.bfloat16),jax.ShapeDtypeStruct(qkv.shape,jnp.bfloat16)),
        in_specs=[vm]*6,out_specs=(vm,vm),
        scratch_shapes=[pltpu.VMEM(go.shape,jnp.bfloat16),pltpu.VMEM((seq,HD),jnp.bfloat16),pltpu.VMEM((seq,HD),jnp.bfloat16),pltpu.VMEM((seq,HD),jnp.float32),pltpu.VMEM((seq,HD),jnp.float32)],
        compiler_params=pltpu.CompilerParams(vmem_limit_bytes=60*2**20),name="attention",
        cost_estimate=pl.CostEstimate(flops=12*go.shape[1]*seq*seq//2,bytes_accessed=12*2**20,transcendentals=0),
    )(qkv,go,cos,sin,segs.reshape(1,seq),segs.reshape(seq,1))

CC = 512
CUT = 5120
PLANE = (("c", "zl", "zh"), (2, 2, 2))
SHEET = (("y", "x"), (4, 4))


def place(axes, sizes, index):
    where = {}
    for axis, size in zip(reversed(axes), reversed(sizes)):
        where[axis] = lax.rem(index, size)
        index = lax.div(index, size)
    return where


def members(group):
    axes, sizes = group
    count = 1
    me = jnp.int32(0)
    for axis, size in zip(axes, sizes):
        count *= size
        me = me * size + lax.axis_index(axis)
    others = [lax.rem(me + k, count) for k in range(1, count)]
    return count, me, others, [place(axes, sizes, other) for other in others]


def scatter_kernel(d_ref, n_ref, wq_ref, wk_ref, wv_ref, x_ref, inv_ref, gain_ref, out_ref, grad_ref, total_ref,
                   w_s, part, ro, rw, rq, rp, n_s, dt_s, mine, g, ry, rz,
                   send, recv, local, psend, precv, ysend, yrecv, nsem,
                   plane, sheet, gsend, grecv):
    x = lax.axis_index("x"); z = lax.axis_index("zh"); o = 1 - z
    c = lax.axis_index("c"); y = lax.axis_index("y"); zl = lax.axis_index("zl")
    right = lax.rem(x + 1, 4); left = lax.rem(x + 3, 4); far = lax.rem(x + 2, 4)
    up = lax.rem(y + 1, 4); down = lax.rem(y + 3, 4); beyond = lax.rem(y + 2, 4)
    to_right = {"x": right}; to_left = {"x": left}; to_z = {"zh": o}
    to_up = {"y": up}; to_down = {"y": down}; to_core = {"c": 1 - c}; to_zl = {"zl": 1 - zl}
    feat = part.shape[3]; half = part.shape[2]
    lo = pl.ds(0, CUT); hi = pl.ds(CUT, feat - CUT)
    wide = wq_ref.shape[1]; narrow = wk_ref.shape[1]
    f32 = jnp.float32; bf = jnp.bfloat16
    loads = [
        pltpu.make_async_copy(wq_ref, w_s.at[:, pl.ds(0, wide)], local.at[0]),
        pltpu.make_async_copy(wk_ref, w_s.at[:, pl.ds(wide, narrow)], local.at[1]),
        pltpu.make_async_copy(wv_ref, w_s.at[:, pl.ds(wide + narrow, narrow)], local.at[2]),
    ]
    for copy in loads:
        copy.start()
    bar = pltpu.get_barrier_semaphore()
    groups = (members(PLANE), members(SHEET))
    everyone = groups[0][3] + groups[1][3]
    for device in everyone:
        pl.semaphore_signal(bar, inc=1, device_id=device, device_id_type=MESH)

    blocks = g.shape[0]
    width = g.shape[2]

    def block_of(i):
        j = lax.div(i, 2)
        return 2 * lax.rem(y + 2 + jnp.where(j == 0, 0, lax.rem(j + 1, 3) + 1), 4) + lax.rem(i, 2)

    def load(i):
        owner = jnp.where(i < blocks, 1 - c, c)
        k = block_of(lax.rem(i, blocks))
        cols = pl.ds(pl.multiple_of((2 * k + owner) * width, width), width)
        s = lax.rem(i, 2)
        return pltpu.make_async_copy(n_ref.at[:, cols], n_s.at[s], nsem.at[s])

    def pair(i):
        k = block_of(i)
        return pltpu.make_async_remote_copy(
            src_ref=mine.at[lax.rem(i, 2)], dst_ref=g.at[k], send_sem=psend.at[i],
            recv_sem=precv.at[i], device_id=to_core, device_id_type=MESH)

    load(jnp.int32(0)).start()
    dt_s[...] = jnp.concatenate([d_ref[s] for s in range(8)], axis=0).T

    def product(i):
        load(i).wait()
        return jnp.dot(dt_s[...], n_s[lax.rem(i, 2)], preferred_element_type=f32)

    def first(i, _):
        load(i + 1).start()

        @pl.when(i >= 2)
        def _():
            pair(i - 2).wait_send()

        mine[lax.rem(i, 2)] = product(i).astype(bf)
        pair(i).start()
        return 0

    def second(i, _):
        @pl.when(i < blocks - 1)
        def _():
            load(i + blocks + 1).start()

        value = product(i + blocks)
        pair(i).wait_recv()
        k = block_of(i)
        g[k] = (value + g[k].astype(f32)).astype(bf)
        return 0

    place_of = (far, right, left, x)

    def piece(rel, sz, j):
        cc = pl.ds(pl.multiple_of(j * CC, CC), CC)
        return cc, lax.dot_general(
            d_ref[2 * place_of[rel] + sz], w_s[cc, :], (((1,), (1,)), ((), ())),
            preferred_element_type=f32).reshape(2, half, CC)

    def compute_other(rel):
        def step(j, _):
            cc, p = piece(rel, o, j)
            part[rel, :, :, cc] = p.astype(bf)
            return 0
        lax.fori_loop(0, feat // CC, step, 0)

    def compute_own(rel, slot):
        def step(j, _):
            cc, p = piece(rel, z, j)
            part[slot, :, :, cc] = p.astype(bf)
            return 0
        lax.fori_loop(0, CUT // CC, step, 0)
        got(12 + rel, rq.at[rel])

        def step2(j, _):
            cc, p = piece(rel, z, j)
            qq = pl.ds(pl.multiple_of(j * CC - CUT, CC), CC)
            part[slot, :, :, cc] = (p + rq[rel, :, :, qq].astype(f32)).astype(bf)
            return 0
        lax.fori_loop(CUT // CC, feat // CC, step2, 0)

    sent = {}

    def go(k, src, dst, dev):
        copy = pltpu.make_async_remote_copy(
            src_ref=src, dst_ref=dst, send_sem=send.at[k], recv_sem=recv.at[k],
            device_id=dev, device_id_type=MESH)
        copy.start()
        sent[k] = copy

    def got(k, ref):
        pltpu.make_async_remote_copy(
            src_ref=ref, dst_ref=ref, send_sem=send.at[k], recv_sem=recv.at[k],
            device_id=to_z, device_id_type=MESH).wait_recv()

    def zsend(rel):
        go(12 + rel, part.at[rel, :, :, hi], rq.at[rel], to_z)

    def free(*keys):
        for k in keys:
            sent.pop(k).wait_send()

    def add(dst, terms, size):
        def step(j, _):
            cc = pl.ds(pl.multiple_of(j * CC, CC), CC)
            acc = terms[0][:, cc].astype(f32)
            for t in terms[1:]:
                acc = acc + t[:, cc].astype(f32)
            dst[:, cc] = acc.astype(bf)
            return 0
        lax.fori_loop(0, size // CC, step, 0)

    ysent = []

    def ygo(k, src, dst, dev):
        copy = pltpu.make_async_remote_copy(
            src_ref=src, dst_ref=dst, send_sem=ysend.at[k], recv_sem=yrecv.at[k],
            device_id=dev, device_id_type=MESH)
        copy.start()
        ysent.append(copy)

    def ygot(k, ref):
        pltpu.make_async_remote_copy(
            src_ref=ref, dst_ref=ref, send_sem=ysend.at[k], recv_sem=yrecv.at[k],
            device_id=to_up, device_id_type=MESH).wait_recv()

    for copy in loads:
        copy.wait()
    compute_other(0)
    pl.semaphore_wait(bar, len(everyone))
    go(0, part.at[0, 0, :, lo], ro.at[0], to_right); go(1, part.at[0, 1, :, lo], ro.at[1], to_left); zsend(0)
    compute_other(1); go(2, part.at[1, 1, :, lo], ro.at[2], to_right); zsend(1)
    compute_other(2); go(3, part.at[2, 0, :, lo], ro.at[3], to_left); zsend(2)
    compute_other(3); zsend(3)
    got(0, ro.at[0]); add(part.at[1, 0], [part.at[1, 0], ro.at[0]], CUT); go(4, part.at[1, 0, :, lo], ro.at[4], to_right)
    got(1, ro.at[1]); add(part.at[2, 1], [part.at[2, 1], ro.at[1]], CUT); go(5, part.at[2, 1, :, lo], ro.at[5], to_left)
    lax.fori_loop(0, blocks, first, 0)
    compute_own(0, 4)
    go(6, part.at[4, 0], rw.at[0], to_right); go(7, part.at[4, 1], rw.at[1], to_left)
    lax.fori_loop(0, 2, second, 0)
    ygo(0, g.at[2 * beyond], ry.at[0], to_up); ygo(1, g.at[2 * beyond + 1], ry.at[1], to_down)
    lax.fori_loop(2, 6, second, 0)
    ygo(2, g.at[2 * up + 1], ry.at[2], to_up); ygo(3, g.at[2 * down], ry.at[3], to_down)
    lax.fori_loop(6, 8, second, 0)
    got(3, ro.at[3]); got(4, ro.at[4]); add(part.at[3, 0], [part.at[3, 0], ro.at[4], ro.at[3]], CUT); go(16, part.at[3, 0, :, lo], rp.at[0], to_z)
    got(2, ro.at[2]); got(5, ro.at[5]); add(part.at[3, 1], [part.at[3, 1], ro.at[5], ro.at[2]], CUT); go(17, part.at[3, 1, :, lo], rp.at[1], to_z)
    compute_own(1, 5); go(8, part.at[5, 1], rw.at[2], to_right)
    ygot(0, ry.at[0]); add(g.at[2 * up], [g.at[2 * up], ry.at[0]], width); ygo(4, g.at[2 * up], ry.at[4], to_up)
    ygot(1, ry.at[1]); add(g.at[2 * down + 1], [g.at[2 * down + 1], ry.at[1]], width); ygo(5, g.at[2 * down + 1], ry.at[5], to_down)
    free(0, 1, 12)
    compute_own(2, 0); go(9, part.at[0, 0], rw.at[3], to_left)
    got(6, rw.at[0]); add(part.at[5, 0], [part.at[5, 0], rw.at[0]], feat); go(10, part.at[5, 0], rw.at[4], to_right)
    got(7, rw.at[1]); add(part.at[0, 1], [part.at[0, 1], rw.at[1]], feat); go(11, part.at[0, 1], rw.at[5], to_left)
    free(2, 4, 13)
    free(3, 5, 14)
    x_load = pltpu.make_async_copy(x_ref, part.at[2], local.at[3])
    x_load.start()
    compute_own(3, 1)
    ygot(3, ry.at[3]); ygot(4, ry.at[4]); add(g.at[2 * y], [g.at[2 * y], ry.at[4], ry.at[3]], width)
    ygot(2, ry.at[2]); ygot(5, ry.at[5]); add(g.at[2 * y + 1], [g.at[2 * y + 1], ry.at[5], ry.at[2]], width)
    ygo(6, g.at[2 * y + 1 - zl], rz, to_zl)

    def final(h, a, b):
        inv = inv_ref[h]

        def step(with_z, j, acc):
            cc = pl.ds(pl.multiple_of(j * CC, CC), CC)
            nd = (part[1, h, :, cc].astype(f32) + rw[a, :, cc].astype(f32) + rw[b, :, cc].astype(f32))
            if with_z:
                nd = nd + rp[h, :, cc].astype(f32)
            part[1, h, :, cc] = nd.astype(bf)
            nd = nd * (part[2, h, :, cc].astype(f32) * inv)
            where = (me_plane, pl.ds(lax.div(j, 2), 1), pl.ds(pl.multiple_of(lax.rem(j, 2) * CC, CC), CC))
            term = jnp.sum(nd, axis=0, keepdims=True)
            if h:
                term = term + plane[where]
            plane[where] = term
            nd = nd * gain_ref[0:1, cc]
            for q in range(CC // 128):
                acc = acc + nd[:, q * 128:(q + 1) * 128]
            return acc

        acc = jnp.zeros((half, 128), f32)
        acc = lax.fori_loop(0, CUT // CC, lambda j, v: step(True, j, v), acc)
        acc = lax.fori_loop(CUT // CC, feat // CC, lambda j, v: step(False, j, v), acc)
        return jnp.sum(acc, axis=1, keepdims=True) * (1.0 / feat)

    def input_gradient(h, mean):
        inv = inv_ref[h]

        def step(j, _):
            cc = pl.ds(pl.multiple_of(j * CC, CC), CC)
            nd = part[1, h, :, cc].astype(f32)
            part[1, h, :, cc] = (inv * (nd * gain_ref[0:1, cc] - part[2, h, :, cc].astype(f32) * inv * mean)).astype(bf)
            return 0
        lax.fori_loop(0, feat // CC, step, 0)

    def share(stage, buf):
        count, me, others, devices = groups[stage]
        copies = []
        for k, device in enumerate(devices):
            copy = pltpu.make_async_remote_copy(
                src_ref=buf.at[me], dst_ref=buf.at[me], send_sem=gsend.at[stage, k],
                recv_sem=grecv.at[stage, me], device_id=device, device_id_type=MESH)
            copy.start()
            copies.append(copy)
        return copies

    def gather_sum(stage, buf, copies):
        count, me, others, devices = groups[stage]
        for k, other in enumerate(others):
            pltpu.make_async_remote_copy(
                src_ref=buf.at[other], dst_ref=buf.at[other], send_sem=gsend.at[stage, k],
                recv_sem=grecv.at[stage, other], device_id=devices[k], device_id_type=MESH).wait_recv()
        value = buf[0]
        for k in range(1, count):
            value = value + buf[k]
        for copy in copies:
            copy.wait_send()
        return value

    me_plane, me_sheet = groups[0][1], groups[1][1]
    x_load.wait()
    got(9, rw.at[3]); got(10, rw.at[4]); got(16, rp.at[0]); mean0 = final(0, 4, 3)
    got(8, rw.at[2]); got(11, rw.at[5]); got(17, rp.at[1]); mean1 = final(1, 5, 2)
    copies = share(0, plane)
    input_gradient(0, mean0)
    store0 = pltpu.make_async_copy(part.at[1, 0], out_ref.at[0], local.at[0])
    store0.start()
    value = gather_sum(0, plane, copies)
    sheet[me_sheet] = value
    copies = share(1, sheet)
    input_gradient(1, mean1)
    store1 = pltpu.make_async_copy(part.at[1, 1], out_ref.at[1], local.at[1])
    store1.start()
    total_ref[...] = gather_sum(1, sheet, copies)
    ygot(6, rz); add(grad_ref, [g.at[2 * y + zl], rz], width)
    store0.wait()
    store1.wait()
    for copy in ysent:
        copy.wait_send()
    for i in (blocks - 2, blocks - 1):
        pair(jnp.int32(i)).wait_send()
    free(*list(sent))


def project_scatter(d, normed, wq, wk, wv, x, inverse, gain):
    seq, cols = d.shape; feat = wq.shape[0]; rows = seq // 8; half = rows // 2
    width = feat // 16
    any_ = pl.BlockSpec(memory_space=pl.ANY); vm = pl.BlockSpec(memory_space=pltpu.VMEM)
    bf = jnp.bfloat16
    dma = pltpu.SemaphoreType.DMA
    out, grad, total = pl.pallas_call(
        scatter_kernel,
        out_shape=(jax.ShapeDtypeStruct((2, half, feat), bf), jax.ShapeDtypeStruct((cols, width), bf),
                   jax.ShapeDtypeStruct((8, feat // 8), jnp.float32)),
        in_specs=[vm] + [any_] * 5 + [vm] * 2, out_specs=(any_, vm, vm),
        scratch_shapes=[
            pltpu.VMEM((feat, cols), bf), pltpu.VMEM((6, 2, half, feat), bf),
            pltpu.VMEM((6, half, CUT), bf), pltpu.VMEM((6, half, feat), bf),
            pltpu.VMEM((4, 2, half, feat - CUT), bf), pltpu.VMEM((2, half, CUT), bf),
            pltpu.VMEM((2, seq, width), bf), pltpu.VMEM((cols, seq), bf),
            pltpu.VMEM((2, cols, width), bf), pltpu.VMEM((8, cols, width), bf),
            pltpu.VMEM((6, cols, width), bf), pltpu.VMEM((cols, width), bf),
            dma((18,)), dma((18,)), dma((4,)), dma((8,)), dma((8,)), dma((7,)), dma((7,)), dma((2,)),
            pltpu.VMEM((8, 8, feat // 8), jnp.float32), pltpu.VMEM((16, 8, feat // 8), jnp.float32),
            dma((2, 16)), dma((2, 16)),
        ],
        compiler_params=pltpu.CompilerParams(collective_id=2, has_side_effects=True, vmem_limit_bytes=63 * 2**20),
        name="project_scatter",
        cost_estimate=pl.CostEstimate(flops=4 * seq * feat * cols, bytes_accessed=48 * 2**20, transcendentals=0),
    )(d.reshape(8, rows, cols), normed, wq, wk, wv,
      x.reshape(2, half, feat), inverse.reshape(2, half, 1), gain.reshape(1, feat))
    return out.reshape(rows, feat), grad, total.reshape(feat)


def rope_tables(segment_row):
    length = segment_row.shape[0]
    earlier = (segment_row[None, :] < segment_row[:, None]).astype(jnp.int32)
    offset = jnp.arange(length, dtype=jnp.int32) - jnp.sum(earlier, axis=1)
    half_dim = HD // 2
    inverse_freq = rope_base ** (-(jnp.arange(half_dim, dtype=jnp.float32) * 2.0 / HD))
    angle = offset.astype(jnp.float32)[:, None] * inverse_freq[None, :]
    cosine, sine = jnp.cos(angle), jnp.sin(angle)
    return jnp.concatenate([cosine, cosine], axis=1), jnp.concatenate([-sine, sine], axis=1)


def body(x_tokens, segment_ids, attended_grad, norm_gain, w_query, w_key, w_value):
    segment_row = segment_ids[0]
    as_float = x_tokens.astype(jnp.float32)
    inverse = lax.rsqrt(jnp.mean(as_float * as_float, axis=1, keepdims=True) + epsilon)
    own = (as_float * inverse * norm_gain).astype(jnp.bfloat16)
    qkv, normed = gather_project(own, w_query, w_key, w_value)
    cosine, sine = rope_tables(segment_row)
    attended, heads_d = attention(qkv, attended_grad, cosine, sine, segment_row)
    input_grad, merged, gain_grad = project_scatter(
        heads_d, normed, w_query, w_key, w_value, x_tokens, inverse, norm_gain
    )
    merged = merged.T.astype(jnp.float32)
    query_cols, key_cols = w_query.shape[1], w_key.shape[1]
    return (
        attended,
        input_grad,
        gain_grad,
        merged[:, :query_cols],
        merged[:, query_cols : query_cols + key_cols],
        merged[:, query_cols + key_cols :],
    )


def solution(mesh):
    torus = Mesh(mesh.devices.reshape(4, 2, 2, 4, 2), DP_TP)
    return jax.shard_map(
        body,
        mesh=torus,
        in_specs=(
            P(DP_TP, None),
            P(DP, None),
            P(DP, TP),
            P(),
            P(None, TP),
            P(None, TP),
            P(None, TP),
        ),
        out_specs=(P(DP, TP), P(DP_TP, None), P(), P(DP, TP), P(DP, TP), P(DP, TP)),
        check_vma=False,
    )
```

```python
import jax
import jax.numpy as jnp
from jax import lax
from jax.experimental import pallas as pl
from jax.experimental.pallas import tpu as pltpu
from jax.sharding import Mesh
from jax.sharding import PartitionSpec as P

HD = 128
SPLIT = 4608
MESH = pl.DeviceIdType.MESH
TP = ("x", "zh")
DP = ("y", "zl", "c")
DP_TP = ("y", "zl", "c", "x", "zh")
epsilon = 1e-05
rope_base = 500000.0
def gather_kernel(n_ref, wq_ref, wk_ref, wv_ref, qkv_ref, full_ref, a_s, w_s, send, recv, local):
    x=lax.axis_index("x"); z=lax.axis_index("zh")
    right=lax.rem(x+1,4); left=lax.rem(x+3,4); far=lax.rem(x+2,4)
    to_right={"x":right}; to_left={"x":left}; to_z={"zh":1-z}
    half=a_s.shape[2]; rows=2*half
    lo=pl.ds(0,SPLIT); hi=pl.ds(SPLIT,a_s.shape[3]-SPLIT); every=pl.ds(0,a_s.shape[3])
    own=pltpu.make_async_copy(n_ref,a_s.at[2*x+z],local.at[0]); own.start()
    bar=pltpu.get_barrier_semaphore()
    for dev in (to_right,to_left,to_z):
        pl.semaphore_signal(bar,inc=1,device_id=dev,device_id_type=MESH)
    own.wait()
    pl.semaphore_wait(bar,3)
    wide=wq_ref.shape[1]; narrow=wk_ref.shape[1]
    loads=[pltpu.make_async_copy(wq_ref,w_s.at[:,pl.ds(0,wide)],local.at[1]),
           pltpu.make_async_copy(wk_ref,w_s.at[:,pl.ds(wide,narrow)],local.at[2]),
           pltpu.make_async_copy(wv_ref,w_s.at[:,pl.ds(wide+narrow,narrow)],local.at[3])]
    sent=[]
    def copy(k,sx,sz,h,cols,dev):
        ref=a_s.at[2*sx+sz,h,:,cols]
        return pltpu.make_async_remote_copy(src_ref=ref,dst_ref=ref,send_sem=send.at[k],recv_sem=recv.at[k],device_id=dev,device_id_type=MESH)
    def go(k,sx,sz,h,cols,dev):
        c=copy(k,sx,sz,h,cols,dev); c.start(); sent.append(c)
    def got(k,sx,sz,h,cols):
        copy(k,sx,sz,h,cols,to_z).wait_recv()
    o=1-z
    go(0,x,z,0,every,to_right); go(1,x,z,1,every,to_left)
    go(6,x,z,0,lo,to_z); go(7,x,z,1,lo,to_z)
    go(2,x,z,1,every,to_right); go(3,x,z,0,every,to_left)
    go(8,x,z,0,hi,to_z); go(9,x,z,1,hi,to_z)
    for c in loads: c.start()
    outs=[]
    def done(i,sx,sz):
        c=pltpu.make_async_copy(a_s.at[2*sx+sz],full_ref.at[2*sx+sz],local.at[4+i]); c.start(); outs.append(c)
    def project(slots):
        def one(i,_):
            s=slots(i)
            r=pl.ds(pl.multiple_of(s*rows,rows),rows)
            def part(j,_):
                kk=pl.ds(pl.multiple_of(j*KC,KC),KC)
                p=lax.dot_general(a_s[s,:,:,kk].reshape(rows,KC),w_s[kk,:],(((1,),(0,)),((),())),preferred_element_type=jnp.float32)
                qkv_ref[r,:]=jnp.where(j==0,p,qkv_ref[r,:]+p)
                return 0
            lax.fori_loop(0,a_s.shape[3]//KC,part,0)
            return 0
        return one
    KC=2048
    def run(n,f): lax.fori_loop(0,n,project(f),0)
    done(0,x,z)
    for c in loads: c.wait()
    run(1,lambda i: 2*x+z)
    got(0,left,z,0,every); go(4,left,z,0,every,to_right); go(10,left,z,0,hi,to_z)
    got(1,right,z,1,every); go(5,right,z,1,every,to_left); go(11,right,z,1,hi,to_z)
    got(6,x,o,0,lo); go(12,x,o,0,lo,to_right); got(7,x,o,1,lo); go(13,x,o,1,lo,to_left)
    go(14,x,o,1,lo,to_right); go(15,x,o,0,lo,to_left)
    got(2,left,z,1,every); go(16,left,z,1,hi,to_z)
    got(3,right,z,0,every); go(17,right,z,0,hi,to_z)
    done(1,left,z); done(2,right,z)
    got(8,x,o,0,hi); got(9,x,o,1,hi); done(3,x,o)
    run(2,lambda i: 2*lax.rem(x+1+2*i,4)+z)
    got(4,far,z,0,every); go(18,far,z,0,hi,to_z)
    got(5,far,z,1,every); go(19,far,z,1,hi,to_z)
    done(4,far,z)
    run(1,lambda i: 2*x+o)
    got(12,left,o,0,lo); go(20,left,o,0,lo,to_right)
    got(13,right,o,1,lo); go(21,right,o,1,lo,to_left)
    run(1,lambda i: 2*far+z)
    got(10,left,o,0,hi); got(11,right,o,1,hi)
    got(14,left,o,1,lo); got(16,left,o,1,hi); done(5,left,o)
    got(15,right,o,0,lo); got(17,right,o,0,hi); done(6,right,o)
    run(2,lambda i: 2*lax.rem(x+1+2*i,4)+o)
    got(20,far,o,0,lo); got(21,far,o,1,lo); got(18,far,o,0,hi); got(19,far,o,1,hi); done(7,far,o)
    run(1,lambda i: 2*far+o)
    for c in sent: c.wait_send()
    for c in outs: c.wait()

def gather_project(normed,wq,wk,wv):
    rows,feat=normed.shape
    cols=wq.shape[1]+2*wk.shape[1]
    any_=pl.BlockSpec(memory_space=pl.ANY); vm=pl.BlockSpec(memory_space=pltpu.VMEM)
    qkv,full=pl.pallas_call(gather_kernel,
        out_shape=(jax.ShapeDtypeStruct((8*rows,cols),jnp.float32),jax.ShapeDtypeStruct((8,2,rows//2,feat),jnp.bfloat16)),
        in_specs=[any_]*4,out_specs=(vm,any_),
        scratch_shapes=[pltpu.VMEM((8,2,rows//2,feat),jnp.bfloat16),pltpu.VMEM((feat,cols),jnp.bfloat16),
            pltpu.SemaphoreType.DMA((22,)),pltpu.SemaphoreType.DMA((22,)),pltpu.SemaphoreType.DMA((12,))],
        compiler_params=pltpu.CompilerParams(collective_id=1,has_side_effects=True,vmem_limit_bytes=60*2**20),name="gather_project",
        cost_estimate=pl.CostEstimate(flops=2*8*rows*feat*cols,bytes_accessed=48*2**20,transcendentals=0),
    )(normed.reshape(2,rows//2,feat),wq,wk,wv)
    return qkv,full.reshape(8*rows,feat)
BQ=256
def _nt(a,b): return lax.dot_general(a,b,(((1,),(1,)),((),())),preferred_element_type=jnp.float32)
def _tn(a,b): return lax.dot_general(a,b,(((0,),(0,)),((),())),preferred_element_type=jnp.float32)
def _nn(a,b): return lax.dot_general(a,b,(((1,),(0,)),((),())),preferred_element_type=jnp.float32)

def attention_kernel(qkv_ref, go_ref, cos_ref, sin_ref, segr_ref, segc_ref, att_ref, d_ref, q_s, k_s, v_s, dk_s, dv_s):
    seq=qkv_ref.shape[0]; heads=go_ref.shape[1]//HD; width=heads*HD
    scale=float(HD)**-0.5
    def rope(u,c,s): return u*c+pltpu.roll(u,HD//2,1)*s
    nb=seq//BQ
    for b in range(nb):
        r=slice(b*BQ,(b+1)*BQ)
        c=cos_ref[r,:]; s=sin_ref[r,:]
        for h in range(heads):
            q_s[r,h*HD:(h+1)*HD]=rope(qkv_ref[r,h*HD:(h+1)*HD],c,s).astype(jnp.bfloat16)
        k_s[r,:]=rope(qkv_ref[r,width:width+HD],c,s).astype(jnp.bfloat16)
        v_s[r,:]=qkv_ref[r,width+HD:width+2*HD].astype(jnp.bfloat16)
    dk_s[...]=jnp.zeros_like(dk_s)
    dv_s[...]=jnp.zeros_like(dv_s)
    for b in range(nb):
        r=slice(b*BQ,(b+1)*BQ)
        lo=max(0,(b*BQ-511)//BQ*BQ); hi=(b+1)*BQ
        kr=slice(lo,hi)
        rows=lax.broadcasted_iota(jnp.int32,(BQ,hi-lo),0)+b*BQ
        cols=lax.broadcasted_iota(jnp.int32,(BQ,hi-lo),1)+lo
        mask=(cols<=rows)&(segr_ref[0:1,kr]==segc_ref[r,0:1])
        def head(h,_):
            hs=pl.ds(pl.multiple_of(h*HD,HD),HD)
            q=q_s[r,hs]; go=go_ref[r,hs]
            k=k_s[kr,:]; v=v_s[kr,:]
            sc=jnp.where(mask,_nt(q,k)*scale,-1e30)
            m=jnp.max(sc,axis=1,keepdims=True)
            e=jnp.exp(sc-m)
            p=e*(1.0/jnp.sum(e,axis=1,keepdims=True))
            w=p.astype(jnp.bfloat16)
            o=_nn(w,v).astype(jnp.bfloat16)
            att_ref[r,hs]=o
            delta=jnp.sum(go.astype(jnp.float32)*o.astype(jnp.float32),axis=1,keepdims=True)
            dv_s[kr,:]+=_tn(w,go)
            dp=_nt(go,v)
            ds=(p*(dp-delta)*scale).astype(jnp.bfloat16)
            dq=_nn(ds,k)
            d_ref[r,hs]=rope(dq,cos_ref[r,:],-sin_ref[r,:]).astype(jnp.bfloat16)
            dk_s[kr,:]+=_tn(ds,q)
            return 0
        lax.fori_loop(0,heads,head,0,unroll=True)
    d_ref[:,width:width+HD]=rope(dk_s[...],cos_ref[...],-sin_ref[...]).astype(jnp.bfloat16)
    d_ref[:,width+HD:width+2*HD]=dv_s[...].astype(jnp.bfloat16)

def attention(qkv,go,cos,sin,segs):
    seq=qkv.shape[0]
    vm=pl.BlockSpec(memory_space=pltpu.VMEM)
    return pl.pallas_call(attention_kernel,
        out_shape=(jax.ShapeDtypeStruct(go.shape,jnp.bfloat16),jax.ShapeDtypeStruct(qkv.shape,jnp.bfloat16)),
        in_specs=[vm]*6,out_specs=(vm,vm),
        scratch_shapes=[pltpu.VMEM(go.shape,jnp.bfloat16),pltpu.VMEM((seq,HD),jnp.bfloat16),pltpu.VMEM((seq,HD),jnp.bfloat16),pltpu.VMEM((seq,HD),jnp.float32),pltpu.VMEM((seq,HD),jnp.float32)],
        compiler_params=pltpu.CompilerParams(vmem_limit_bytes=60*2**20),name="attention",
        cost_estimate=pl.CostEstimate(flops=12*go.shape[1]*seq*seq//2,bytes_accessed=12*2**20,transcendentals=0),
    )(qkv,go,cos,sin,segs.reshape(1,seq),segs.reshape(seq,1))

CC = 512
CUT = 5120
PLANE = (("c", "zl", "zh"), (2, 2, 2))
SHEET = (("y", "x"), (4, 4))


def place(axes, sizes, index):
    where = {}
    for axis, size in zip(reversed(axes), reversed(sizes)):
        where[axis] = lax.rem(index, size)
        index = lax.div(index, size)
    return where


def members(group):
    axes, sizes = group
    count = 1
    me = jnp.int32(0)
    for axis, size in zip(axes, sizes):
        count *= size
        me = me * size + lax.axis_index(axis)
    others = [lax.rem(me + k, count) for k in range(1, count)]
    return count, me, others, [place(axes, sizes, other) for other in others]


def scatter_kernel(d_ref, n_ref, wq_ref, wk_ref, wv_ref, x_ref, inv_ref, gain_ref, out_ref, grad_ref, total_ref,
                   w_s, part, ro, rw, rq, rp, n_s, dt_s, mine, g, ry, rz,
                   send, recv, local, psend, precv, ysend, yrecv, nsem,
                   plane, sheet, gsend, grecv, wsem):
    x = lax.axis_index("x"); z = lax.axis_index("zh"); o = 1 - z
    c = lax.axis_index("c"); y = lax.axis_index("y"); zl = lax.axis_index("zl")
    right = lax.rem(x + 1, 4); left = lax.rem(x + 3, 4); far = lax.rem(x + 2, 4)
    up = lax.rem(y + 1, 4); down = lax.rem(y + 3, 4); beyond = lax.rem(y + 2, 4)
    to_right = {"x": right}; to_left = {"x": left}; to_z = {"zh": o}
    to_up = {"y": up}; to_down = {"y": down}; to_core = {"c": 1 - c}; to_zl = {"zl": 1 - zl}
    feat = part.shape[3]; half = part.shape[2]
    lo = pl.ds(0, CUT); hi = pl.ds(CUT, feat - CUT)
    wide = wq_ref.shape[1]; narrow = wk_ref.shape[1]
    f32 = jnp.float32; bf = jnp.bfloat16
    def w_loads(j):
        rr = pl.ds(pl.multiple_of(j * CC, CC), CC)
        return (
            pltpu.make_async_copy(wq_ref.at[rr], w_s.at[rr, pl.ds(0, wide)], wsem.at[0, j]),
            pltpu.make_async_copy(wk_ref.at[rr], w_s.at[rr, pl.ds(wide, narrow)], wsem.at[1, j]),
            pltpu.make_async_copy(wv_ref.at[rr], w_s.at[rr, pl.ds(wide + narrow, narrow)], wsem.at[2, j]),
        )

    def w_start(j, _):
        for copy in w_loads(j):
            copy.start()
        return 0

    lax.fori_loop(0, feat // CC, w_start, 0)
    bar = pltpu.get_barrier_semaphore()
    groups = (members(PLANE), members(SHEET))
    everyone = groups[0][3] + groups[1][3]
    for device in everyone:
        pl.semaphore_signal(bar, inc=1, device_id=device, device_id_type=MESH)

    blocks = g.shape[0]
    width = g.shape[2]

    def block_of(i):
        j = lax.div(i, 2)
        return 2 * lax.rem(y + 2 + jnp.where(j == 0, 0, lax.rem(j + 1, 3) + 1), 4) + lax.rem(i, 2)

    def load(i):
        owner = jnp.where(i < blocks, 1 - c, c)
        k = block_of(lax.rem(i, blocks))
        cols = pl.ds(pl.multiple_of((2 * k + owner) * width, width), width)
        s = lax.rem(i, 2)
        return pltpu.make_async_copy(n_ref.at[:, cols], n_s.at[s], nsem.at[s])

    def pair(i):
        k = block_of(i)
        return pltpu.make_async_remote_copy(
            src_ref=mine.at[lax.rem(i, 2)], dst_ref=g.at[k], send_sem=psend.at[i],
            recv_sem=precv.at[i], device_id=to_core, device_id_type=MESH)

    load(jnp.int32(0)).start()
    dt_s[...] = jnp.concatenate([d_ref[s] for s in range(8)], axis=0).T

    def product(i):
        load(i).wait()
        return jnp.dot(dt_s[...], n_s[lax.rem(i, 2)], preferred_element_type=f32)

    def first(i, _):
        load(i + 1).start()

        @pl.when(i >= 2)
        def _():
            pair(i - 2).wait_send()

        mine[lax.rem(i, 2)] = product(i).astype(bf)
        pair(i).start()
        return 0

    def second(i, _):
        @pl.when(i < blocks - 1)
        def _():
            load(i + blocks + 1).start()

        value = product(i + blocks)
        pair(i).wait_recv()
        k = block_of(i)
        g[k] = (value + g[k].astype(f32)).astype(bf)
        return 0

    place_of = (far, right, left, x)

    def piece(rel, sz, j):
        cc = pl.ds(pl.multiple_of(j * CC, CC), CC)
        return cc, lax.dot_general(
            d_ref[2 * place_of[rel] + sz], w_s[cc, :], (((1,), (1,)), ((), ())),
            preferred_element_type=f32).reshape(2, half, CC)

    def compute_other(rel):
        def step(j, _):
            if rel == 0:
                for copy in w_loads(j):
                    copy.wait()
            cc, p = piece(rel, o, j)
            part[rel, :, :, cc] = p.astype(bf)
            return 0
        lax.fori_loop(0, feat // CC, step, 0)

    def compute_own(rel, slot):
        def step(j, _):
            cc, p = piece(rel, z, j)
            part[slot, :, :, cc] = p.astype(bf)
            return 0
        lax.fori_loop(0, CUT // CC, step, 0)
        got(12 + rel, rq.at[rel])

        def step2(j, _):
            cc, p = piece(rel, z, j)
            qq = pl.ds(pl.multiple_of(j * CC - CUT, CC), CC)
            part[slot, :, :, cc] = (p + rq[rel, :, :, qq].astype(f32)).astype(bf)
            return 0
        lax.fori_loop(CUT // CC, feat // CC, step2, 0)

    sent = {}

    def go(k, src, dst, dev):
        copy = pltpu.make_async_remote_copy(
            src_ref=src, dst_ref=dst, send_sem=send.at[k], recv_sem=recv.at[k],
            device_id=dev, device_id_type=MESH)
        copy.start()
        sent[k] = copy

    def got(k, ref):
        pltpu.make_async_remote_copy(
            src_ref=ref, dst_ref=ref, send_sem=send.at[k], recv_sem=recv.at[k],
            device_id=to_z, device_id_type=MESH).wait_recv()

    def zsend(rel):
        go(12 + rel, part.at[rel, :, :, hi], rq.at[rel], to_z)

    def free(*keys):
        for k in keys:
            sent.pop(k).wait_send()

    def add(dst, terms, size):
        def step(j, _):
            cc = pl.ds(pl.multiple_of(j * CC, CC), CC)
            acc = terms[0][:, cc].astype(f32)
            for t in terms[1:]:
                acc = acc + t[:, cc].astype(f32)
            dst[:, cc] = acc.astype(bf)
            return 0
        lax.fori_loop(0, size // CC, step, 0)

    ysent = []

    def ygo(k, src, dst, dev):
        copy = pltpu.make_async_remote_copy(
            src_ref=src, dst_ref=dst, send_sem=ysend.at[k], recv_sem=yrecv.at[k],
            device_id=dev, device_id_type=MESH)
        copy.start()
        ysent.append(copy)

    def ygot(k, ref):
        pltpu.make_async_remote_copy(
            src_ref=ref, dst_ref=ref, send_sem=ysend.at[k], recv_sem=yrecv.at[k],
            device_id=to_up, device_id_type=MESH).wait_recv()

    compute_other(0)
    pl.semaphore_wait(bar, len(everyone))
    go(0, part.at[0, 0, :, lo], ro.at[0], to_right); go(1, part.at[0, 1, :, lo], ro.at[1], to_left); zsend(0)
    compute_other(1); go(2, part.at[1, 1, :, lo], ro.at[2], to_right); zsend(1)
    compute_other(2); go(3, part.at[2, 0, :, lo], ro.at[3], to_left); zsend(2)
    compute_other(3); zsend(3)
    got(0, ro.at[0]); add(part.at[1, 0], [part.at[1, 0], ro.at[0]], CUT); go(4, part.at[1, 0, :, lo], ro.at[4], to_right)
    got(1, ro.at[1]); add(part.at[2, 1], [part.at[2, 1], ro.at[1]], CUT); go(5, part.at[2, 1, :, lo], ro.at[5], to_left)
    lax.fori_loop(0, blocks, first, 0)
    compute_own(0, 4)
    go(6, part.at[4, 0], rw.at[0], to_right); go(7, part.at[4, 1], rw.at[1], to_left)
    lax.fori_loop(0, 2, second, 0)
    ygo(0, g.at[2 * beyond], ry.at[0], to_up); ygo(1, g.at[2 * beyond + 1], ry.at[1], to_down)
    lax.fori_loop(2, 6, second, 0)
    ygo(2, g.at[2 * up + 1], ry.at[2], to_up); ygo(3, g.at[2 * down], ry.at[3], to_down)
    lax.fori_loop(6, 8, second, 0)
    got(3, ro.at[3]); got(4, ro.at[4]); add(part.at[3, 0], [part.at[3, 0], ro.at[4], ro.at[3]], CUT); go(16, part.at[3, 0, :, lo], rp.at[0], to_z)
    got(2, ro.at[2]); got(5, ro.at[5]); add(part.at[3, 1], [part.at[3, 1], ro.at[5], ro.at[2]], CUT); go(17, part.at[3, 1, :, lo], rp.at[1], to_z)
    compute_own(1, 5); go(8, part.at[5, 1], rw.at[2], to_right)
    ygot(0, ry.at[0]); add(g.at[2 * up], [g.at[2 * up], ry.at[0]], width); ygo(4, g.at[2 * up], ry.at[4], to_up)
    ygot(1, ry.at[1]); add(g.at[2 * down + 1], [g.at[2 * down + 1], ry.at[1]], width); ygo(5, g.at[2 * down + 1], ry.at[5], to_down)
    free(0, 1, 12)
    compute_own(2, 0); go(9, part.at[0, 0], rw.at[3], to_left)
    got(6, rw.at[0]); add(part.at[5, 0], [part.at[5, 0], rw.at[0]], feat); go(10, part.at[5, 0], rw.at[4], to_right)
    got(7, rw.at[1]); add(part.at[0, 1], [part.at[0, 1], rw.at[1]], feat); go(11, part.at[0, 1], rw.at[5], to_left)
    free(2, 4, 13)
    free(3, 5, 14)
    x_load = pltpu.make_async_copy(x_ref, part.at[2], local.at[3])
    x_load.start()
    compute_own(3, 1)
    ygot(3, ry.at[3]); ygot(4, ry.at[4]); add(g.at[2 * y], [g.at[2 * y], ry.at[4], ry.at[3]], width)
    ygot(2, ry.at[2]); ygot(5, ry.at[5]); add(g.at[2 * y + 1], [g.at[2 * y + 1], ry.at[5], ry.at[2]], width)
    ygo(6, g.at[2 * y + 1 - zl], rz, to_zl)

    def final(h, a, b):
        inv = inv_ref[h]

        def step(with_z, j, acc):
            cc = pl.ds(pl.multiple_of(j * CC, CC), CC)
            nd = (part[1, h, :, cc].astype(f32) + rw[a, :, cc].astype(f32) + rw[b, :, cc].astype(f32))
            if with_z:
                nd = nd + rp[h, :, cc].astype(f32)
            part[1, h, :, cc] = nd.astype(bf)
            nd = nd * (part[2, h, :, cc].astype(f32) * inv)
            where = (me_plane, pl.ds(lax.div(j, 2), 1), pl.ds(pl.multiple_of(lax.rem(j, 2) * CC, CC), CC))
            term = jnp.sum(nd, axis=0, keepdims=True)
            if h:
                term = term + plane[where]
            plane[where] = term
            nd = nd * gain_ref[0:1, cc]
            for q in range(CC // 128):
                acc = acc + nd[:, q * 128:(q + 1) * 128]
            return acc

        acc = jnp.zeros((half, 128), f32)
        acc = lax.fori_loop(0, CUT // CC, lambda j, v: step(True, j, v), acc)
        acc = lax.fori_loop(CUT // CC, feat // CC, lambda j, v: step(False, j, v), acc)
        return jnp.sum(acc, axis=1, keepdims=True) * (1.0 / feat)

    def input_gradient(h, mean):
        inv = inv_ref[h]

        def step(j, _):
            cc = pl.ds(pl.multiple_of(j * CC, CC), CC)
            nd = part[1, h, :, cc].astype(f32)
            part[1, h, :, cc] = (inv * (nd * gain_ref[0:1, cc] - part[2, h, :, cc].astype(f32) * inv * mean)).astype(bf)
            return 0
        lax.fori_loop(0, feat // CC, step, 0)

    def share(stage, buf):
        count, me, others, devices = groups[stage]
        copies = []
        for k, device in enumerate(devices):
            copy = pltpu.make_async_remote_copy(
                src_ref=buf.at[me], dst_ref=buf.at[me], send_sem=gsend.at[stage, k],
                recv_sem=grecv.at[stage, me], device_id=device, device_id_type=MESH)
            copy.start()
            copies.append(copy)
        return copies

    def gather_sum(stage, buf, copies):
        count, me, others, devices = groups[stage]
        for k, other in enumerate(others):
            pltpu.make_async_remote_copy(
                src_ref=buf.at[other], dst_ref=buf.at[other], send_sem=gsend.at[stage, k],
                recv_sem=grecv.at[stage, other], device_id=devices[k], device_id_type=MESH).wait_recv()
        value = buf[0]
        for k in range(1, count):
            value = value + buf[k]
        for copy in copies:
            copy.wait_send()
        return value

    me_plane, me_sheet = groups[0][1], groups[1][1]
    x_load.wait()
    got(9, rw.at[3]); got(10, rw.at[4]); got(16, rp.at[0]); mean0 = final(0, 4, 3)
    got(8, rw.at[2]); got(11, rw.at[5]); got(17, rp.at[1]); mean1 = final(1, 5, 2)
    copies = share(0, plane)
    input_gradient(0, mean0)
    store0 = pltpu.make_async_copy(part.at[1, 0], out_ref.at[0], local.at[0])
    store0.start()
    value = gather_sum(0, plane, copies)
    sheet[me_sheet] = value
    copies = share(1, sheet)
    input_gradient(1, mean1)
    store1 = pltpu.make_async_copy(part.at[1, 1], out_ref.at[1], local.at[1])
    store1.start()
    total_ref[...] = gather_sum(1, sheet, copies)
    ygot(6, rz); add(grad_ref, [g.at[2 * y + zl], rz], width)
    store0.wait()
    store1.wait()
    for copy in ysent:
        copy.wait_send()
    for i in (blocks - 2, blocks - 1):
        pair(jnp.int32(i)).wait_send()
    free(*list(sent))


def project_scatter(d, normed, wq, wk, wv, x, inverse, gain):
    seq, cols = d.shape; feat = wq.shape[0]; rows = seq // 8; half = rows // 2
    width = feat // 16
    any_ = pl.BlockSpec(memory_space=pl.ANY); vm = pl.BlockSpec(memory_space=pltpu.VMEM)
    bf = jnp.bfloat16
    dma = pltpu.SemaphoreType.DMA
    out, grad, total = pl.pallas_call(
        scatter_kernel,
        out_shape=(jax.ShapeDtypeStruct((2, half, feat), bf), jax.ShapeDtypeStruct((cols, width), bf),
                   jax.ShapeDtypeStruct((8, feat // 8), jnp.float32)),
        in_specs=[vm] + [any_] * 5 + [vm] * 2, out_specs=(any_, vm, vm),
        scratch_shapes=[
            pltpu.VMEM((feat, cols), bf), pltpu.VMEM((6, 2, half, feat), bf),
            pltpu.VMEM((6, half, CUT), bf), pltpu.VMEM((6, half, feat), bf),
            pltpu.VMEM((4, 2, half, feat - CUT), bf), pltpu.VMEM((2, half, CUT), bf),
            pltpu.VMEM((2, seq, width), bf), pltpu.VMEM((cols, seq), bf),
            pltpu.VMEM((2, cols, width), bf), pltpu.VMEM((8, cols, width), bf),
            pltpu.VMEM((6, cols, width), bf), pltpu.VMEM((cols, width), bf),
            dma((18,)), dma((18,)), dma((4,)), dma((8,)), dma((8,)), dma((7,)), dma((7,)), dma((2,)),
            pltpu.VMEM((8, 8, feat // 8), jnp.float32), pltpu.VMEM((16, 8, feat // 8), jnp.float32),
            dma((2, 16)), dma((2, 16)), dma((3, feat // CC)),
        ],
        compiler_params=pltpu.CompilerParams(collective_id=2, has_side_effects=True, vmem_limit_bytes=63 * 2**20),
        name="project_scatter",
        cost_estimate=pl.CostEstimate(flops=4 * seq * feat * cols, bytes_accessed=48 * 2**20, transcendentals=0),
    )(d.reshape(8, rows, cols), normed, wq, wk, wv,
      x.reshape(2, half, feat), inverse.reshape(2, half, 1), gain.reshape(1, feat))
    return out.reshape(rows, feat), grad, total.reshape(feat)


def rope_tables(segment_row):
    length = segment_row.shape[0]
    earlier = (segment_row[None, :] < segment_row[:, None]).astype(jnp.int32)
    offset = jnp.arange(length, dtype=jnp.int32) - jnp.sum(earlier, axis=1)
    half_dim = HD // 2
    inverse_freq = rope_base ** (-(jnp.arange(half_dim, dtype=jnp.float32) * 2.0 / HD))
    angle = offset.astype(jnp.float32)[:, None] * inverse_freq[None, :]
    cosine, sine = jnp.cos(angle), jnp.sin(angle)
    return jnp.concatenate([cosine, cosine], axis=1), jnp.concatenate([-sine, sine], axis=1)


def body(x_tokens, segment_ids, attended_grad, norm_gain, w_query, w_key, w_value):
    segment_row = segment_ids[0]
    as_float = x_tokens.astype(jnp.float32)
    inverse = lax.rsqrt(jnp.mean(as_float * as_float, axis=1, keepdims=True) + epsilon)
    own = (as_float * inverse * norm_gain).astype(jnp.bfloat16)
    qkv, normed = gather_project(own, w_query, w_key, w_value)
    cosine, sine = rope_tables(segment_row)
    attended, heads_d = attention(qkv, attended_grad, cosine, sine, segment_row)
    input_grad, merged, gain_grad = project_scatter(
        heads_d, normed, w_query, w_key, w_value, x_tokens, inverse, norm_gain
    )
    merged = merged.T.astype(jnp.float32)
    query_cols, key_cols = w_query.shape[1], w_key.shape[1]
    return (
        attended,
        input_grad,
        gain_grad,
        merged[:, :query_cols],
        merged[:, query_cols : query_cols + key_cols],
        merged[:, query_cols + key_cols :],
    )


def solution(mesh):
    torus = Mesh(mesh.devices.reshape(4, 2, 2, 4, 2), DP_TP)
    return jax.shard_map(
        body,
        mesh=torus,
        in_specs=(
            P(DP_TP, None),
            P(DP, None),
            P(DP, TP),
            P(),
            P(None, TP),
            P(None, TP),
            P(None, TP),
        ),
        out_specs=(P(DP, TP), P(DP_TP, None), P(), P(DP, TP), P(DP, TP), P(DP, TP)),
        check_vma=False,
    )
```
